512 devices in a mesh: dp: 128 (over x, z_lo, y), concept: 4 (over z_hi, core).
Axes of the slice: x: 4, y: 4, z: 16 (z_hi: 2, z_lo: 8; z = z_hi * 8 + z_lo), core: 2. Of those that a mesh axis runs over, the one named last changes fastest.
Arguments:
- text: bfloat16 [65536, 1024], P('dp', 'concept'), may hold values from -6 to 6
- concept_table: bfloat16 [393216, 1024], P('dp', 'concept'), may hold values from -6 to 6
- ids: int32 [65536], P('dp'), may hold values from 0 to 393215, as said below
Outputs:
- balanced: float32 [65536], P('dp')
The draws below stay inside these ranges and needn't reach their ends.
Inputs may be any that keep to these rules, and one draw needn't show every extreme that they name: In the 512 pairs of one index of dp, at most 8 ids fall in any one aligned range of 3072 concepts (c * 3072 to (c + 1) * 3072 - 1); in each such block of pairs some range holds exactly 8.
All inputs are finite; a program needn't handle non-finite values.
Results may differ from the reference program's by a relative error of at most 0.0003.
Values may be sent and summed in bfloat16 or wider, within the bound.
A program may use at most 64 MiB of HBM per device.

```python
import jax
import jax.numpy as jnp
from jax import lax

D = 1024
CONC_OWN = 3072
PAIR_DEV = 512
CAP = 16
SLOT = 8
CONCEPTS = 393216
PAIRS = 65536
N_DP = 128


def draw_ids(key, part):
    keys = jax.random.split(jax.random.fold_in(key, 17), N_DP)

    def one_block(block_key):
        first, second, third, fourth = jax.random.split(block_key, 4)
        favoured = jax.random.randint(first, (), 0, N_DP)
        places = jax.random.permutation(second, N_DP * SLOT)
        holders = jnp.arange(N_DP * SLOT, dtype=jnp.int32) // SLOT
        scores = jnp.where(holders == favoured, places - N_DP * SLOT, places)
        order = jnp.argsort(scores, stable=True)
        owners = (order[:PAIR_DEV] // SLOT).astype(jnp.int32)
        owners = owners[jax.random.permutation(fourth, PAIR_DEV)]
        raw = jax.random.randint(third, (PAIR_DEV,), 0, CONC_OWN)
        squared = raw * raw // CONC_OWN
        cubed = squared * raw // CONC_OWN
        return (owners * CONC_OWN + cubed).astype(jnp.int32)
    return jax.vmap(one_block)(keys).reshape(-1)


def levels(rng, dims, cuts, smallest, high):
    def one(axis_at, shards_of):
        steps = jax.random.uniform(jax.random.fold_in(jax.random.fold_in(rng, 6), axis_at), (shards_of,), jnp.float32, smallest / len(cuts), high / len(cuts))
        return jnp.repeat(jnp.exp(steps), dims[axis_at] // shards_of).reshape((-1,) + (1,) * (len(dims) - axis_at - 1))

    loudness = one(*cuts[0])
    for cut in cuts[1:]:
        loudness = loudness * one(*cut)
    return loudness


def bell_draw(own_key, shape, width, bound, cuts=(), kind=jnp.bfloat16):
    array = width * jax.random.normal(own_key, shape, jnp.float32)
    if cuts:
        array = array * levels(own_key, shape, cuts, -0.22, 0.18)
    return jnp.clip(array, -bound, bound).astype(kind)


def setup_inputs(seed: int = 0) -> dict:
    splits = jax.random.split(jax.random.key(seed), 4)
    text = bell_draw(splits[0], (PAIRS, D), 1.0, 6.0, ((0, 128), (1, 4)))
    concept_table = bell_draw(splits[1], (CONCEPTS, D), 1.0, 6.0, ((0, 128), (1, 4)))
    ids = draw_ids(jax.random.fold_in(splits[3], 71), 0)
    return {"text": text, "concept_table": concept_table, "ids": ids}


logit_scale = 64.0
epsilon = 1e-06

def reference(text, concept_table, ids):
    text_blocks = text.reshape(N_DP, PAIR_DEV, D)
    id_blocks = ids.reshape(N_DP, PAIR_DEV)

    def one_block(args):
        block_text, block_ids = args
        pieces = jnp.take(concept_table, block_ids, axis=0).astype(jnp.float32)
        floats = block_text.astype(jnp.float32)
        return (lax.optimization_barrier(jnp.sum(floats * pieces, axis=1)), lax.optimization_barrier(jnp.sum(floats * floats, axis=1)), lax.optimization_barrier(jnp.sum(pieces * pieces, axis=1)))
    dot, tsq, csq = lax.map(one_block, (text_blocks, id_blocks))
    dot = dot.reshape(-1)
    tsq = tsq.reshape(-1)
    csq = csq.reshape(-1)
    match = jax.nn.sigmoid(logit_scale * dot * lax.rsqrt(tsq + epsilon) * lax.rsqrt(csq + epsilon))
    count = jnp.zeros((CONCEPTS,), jnp.float32).at[ids].add(match)
    capped = CAP * 1.0
    return match * capped / jnp.maximum(jnp.take(count, ids), capped)
```

```python
import functools

import jax
import jax.numpy as jnp
from jax import lax
from jax.experimental import pallas as pl
from jax.experimental.pallas import tpu as pltpu
from jax.sharding import PartitionSpec as P

CAP = 16
SLOT = 8
NX, NZ, NY = 4, 8, 4
PLANE = NX * NY
ROW = PLANE * SLOT
Z_ORDER = (4, 3, 5, 2, 6, 1, 7)

logit_scale = 64.0
epsilon = 1e-06
MESH = pl.DeviceIdType.MESH


def kernel(
    text_hbm, table_hbm, ids_ref, out_ref,
    text_v, table_v, picks, sent, carried, landed,
    meta_out, meta_mid, meta_tile, meta_in,
    ids_wide, hot, pieces, part_out, part_in,
    back_out, back_mid, back_tile, back_in,
    load_sem, z_send, z_recv, mz_send, mz_recv, mt_send, mt_recv,
    xy_send, xy_recv, part_send, part_recv, bz_send, bz_recv, bt_send, bt_recv,
):
    f32, bf16, i32 = jnp.float32, jnp.bfloat16, jnp.int32
    pairs = ids_ref.shape[1]
    held = table_v.shape[0]
    me = lax.axis_index("dp")
    mine = lax.axis_index("concept")
    my_x, my_z, my_y = me // (NZ * NY), (me // NY) % NZ, me % NY

    def along_z(k):
        return (my_x * (NZ * NY) + ((my_z + k + NZ) % NZ) * NY + my_y, mine)

    def in_plane(j):
        x = (my_x + j // NY) % NX
        y = (my_y + j % NY) % NY
        return (x * (NZ * NY) + my_z * NY + y, mine)

    def in_plane_back(j):
        x = (my_x + NX - j // NY) % NX
        y = (my_y + NY - j % NY) % NY
        return (x * (NZ * NY) + my_z * NY + y, mine)

    def remote(src, dst, send, recv, device):
        return pltpu.make_async_remote_copy(
            src_ref=src, dst_ref=dst, send_sem=send, recv_sem=recv,
            device_id=device, device_id_type=MESH,
        )

    def settle(ref, sem):
        pltpu.make_async_copy(ref, ref, sem).wait()

    load_text = pltpu.make_async_copy(text_hbm, text_v, load_sem.at[0])
    load_text.start()
    load_table = pltpu.make_async_copy(table_hbm, table_v, load_sem.at[1])
    load_table.start()

    barrier = pltpu.get_barrier_semaphore()
    for c in range(1, 4):
        other = (mine // 2 + c // 2) % 2 * 2 + (mine % 2 + c % 2) % 2
        pl.semaphore_signal(barrier, inc=1, device_id=(me, other), device_id_type=MESH)

    def greet_z(k, carry):
        pl.semaphore_signal(barrier, inc=1, device_id=along_z(k), device_id_type=MESH)
        return carry

    def greet_plane(j, carry):
        pl.semaphore_signal(barrier, inc=1, device_id=in_plane(j), device_id_type=MESH)
        return carry

    lax.fori_loop(1, NZ, greet_z, 0)
    lax.fori_loop(1, PLANE, greet_plane, 0)

    ids = ids_ref[...]
    owner = ((ids >> 10) * 43691) >> 17
    local = ids - owner * held
    to_z = (((owner >> 2) & 7) - my_z) & 7
    to_plane = ((((owner >> 5) - my_x) & 3) << 2) | (((owner & 3) - my_y) & 3)
    relative = to_z * PLANE + to_plane
    is_owner = jnp.where(
        lax.broadcasted_iota(i32, (NZ * PLANE, pairs), 0) == relative, 1.0, 0.0
    )
    earlier = jnp.where(
        lax.broadcasted_iota(i32, (pairs, pairs), 0)
        < lax.broadcasted_iota(i32, (pairs, pairs), 1),
        1.0, 0.0,
    ).astype(bf16)
    ahead = jnp.dot(is_owner.astype(bf16), earlier, preferred_element_type=f32)
    rank = jnp.sum(is_owner * ahead, axis=0, keepdims=True).astype(i32)
    lane = to_plane * SLOT + rank
    target = to_z * ROW + lane

    values = jnp.concatenate(
        [
            (local >> 6).astype(f32),
            (local & 63).astype(f32),
            jnp.ones((1, pairs), f32),
            jnp.zeros((5, pairs), f32),
        ],
        axis=0,
    ).astype(bf16)
    rows = lax.broadcasted_iota(i32, (ROW, pairs), 0)
    for k in range(NZ):
        pick = jnp.where(rows + k * ROW == target, 1.0, 0.0).astype(bf16)
        picks[k] = pick
        meta = lax.dot_general(
            values, pick, (((1,), (1,)), ((), ())), preferred_element_type=f32
        )
        meta_out[k] = meta[0:1] * 64.0 + meta[1:2] + meta[2:3] - 1.0

    pl.semaphore_wait(barrier, NZ - 1 + PLANE - 1 + 3)

    for k in Z_ORDER:
        remote(meta_out.at[k], meta_mid.at[k], mz_send, mz_recv, along_z(k)).start()

    load_text.wait()

    def send_z(k):
        remote(sent.at[k], carried.at[k], z_send, z_recv.at[k], along_z(k)).start()

    before = None
    for k in Z_ORDER + (0,):
        block = jnp.dot(picks[k], text_v[...], preferred_element_type=f32)
        sent[k] = block.reshape(PLANE, SLOT, -1).astype(bf16)
        if before is not None:
            send_z(before)
        before = k

    def pass_on(source, k):
        def one(j, carry):
            remote(
                source.at[k, j], landed.at[k, j], xy_send, xy_recv.at[k], in_plane(j)
            ).start()
            return carry
        lax.fori_loop(1, PLANE, one, 0)

    settle(meta_mid.at[pl.ds(1, NZ - 1)], mz_recv)
    meta_tile[...] = jnp.concatenate(
        [meta_out[0]] + [meta_mid[k] for k in range(1, NZ)], axis=0
    )
    pass_on(sent, 0)

    def send_meta(j, carry):
        remote(meta_tile, meta_in.at[j], mt_send, mt_recv, in_plane(j)).start()
        return carry

    lax.fori_loop(1, PLANE, send_meta, 0)
    settle(meta_in.at[pl.ds(1, PLANE - 1)], mt_recv)
    group = lax.broadcasted_iota(i32, (NZ, ROW), 1) // SLOT
    slot_ids = meta_tile[...]
    for j in range(1, PLANE):
        slot_ids = jnp.where(group == j, meta_in[j], slot_ids)

    square = jnp.concatenate([slot_ids, jnp.zeros((ROW - NZ, ROW), f32)], axis=0)
    turned = jnp.transpose(square)
    for k in range(NZ):
        ids_wide[k] = jnp.broadcast_to(turned[:, k : k + 1], (ROW, ROW))

    load_table.wait()
    columns = lax.broadcasted_iota(i32, (ROW, ROW), 1).astype(f32)

    def fetch(k, carry):
        wanted = ids_wide[k]
        for c in range(held // ROW):
            hot[:, c * ROW : (c + 1) * ROW] = jnp.where(
                wanted - float(c * ROW) == columns, 1.0, 0.0
            ).astype(bf16)
        pieces[k] = jnp.dot(hot[...], table_v[...], preferred_element_type=f32)
        return carry

    lax.fori_loop(0, NZ, fetch, 0)

    for k in Z_ORDER:
        settle(carried.at[k], z_recv.at[k])
        pass_on(carried, k)

    at_lane = lax.broadcasted_iota(i32, (ROW, ROW), 1)
    sums = jnp.zeros((ROW, ROW), f32)
    for k in (0,) + Z_ORDER:
        settle(landed.at[k, pl.ds(1, PLANE - 1)], xy_recv.at[k])
        own = (sent if k == 0 else carried)[k, 0:1].astype(f32)
        others = landed[k, 1:PLANE].astype(f32)
        words = jnp.concatenate([own, others], axis=0).reshape(ROW, -1)
        piece = pieces[k]
        for at, product in ((k, words * piece), (NZ + k, words * words), (2 * NZ + k, piece * piece)):
            total = jnp.sum(product, axis=1, keepdims=True)
            sums = jnp.where(at_lane == at, total, sums)
    part_out[...] = jnp.transpose(sums)[0 : 3 * NZ]

    for c in range(1, 4):
        other = (mine // 2 + c // 2) % 2 * 2 + (mine % 2 + c % 2) % 2
        remote(
            part_out, part_in.at[c], part_send, part_recv, (me, other)
        ).start()
    settle(part_in.at[pl.ds(1, 3)], part_recv)
    whole = (part_out[...] + part_in[1]) + (part_in[2] + part_in[3])
    dot, tsq, csq = whole[0:NZ], whole[NZ : 2 * NZ], whole[2 * NZ : 3 * NZ]
    match = jax.nn.sigmoid(
        logit_scale * dot * lax.rsqrt(tsq + epsilon) * lax.rsqrt(csq + epsilon)
    )
    match = jnp.where(slot_ids >= 0.0, match, 0.0)

    match_turned = jnp.transpose(
        jnp.concatenate([match, jnp.zeros((ROW - NZ, ROW), f32)], axis=0)
    )
    counts = [jnp.zeros((SLOT, ROW), f32) for _ in range(NZ)]
    for m in range(NZ):
        weight = jnp.broadcast_to(match_turned[:, m : m + 1], (ROW, ROW))
        theirs = ids_wide[m]
        for k in range(NZ):
            same = jnp.where(theirs == slot_ids[k : k + 1], weight, 0.0)
            counts[k] = counts[k] + jnp.sum(same.reshape(ROW // SLOT, SLOT, ROW), axis=0)
    count = jnp.concatenate([jnp.sum(c, axis=0, keepdims=True) for c in counts], axis=0)
    capped = CAP * 1.0
    balanced = match * capped / jnp.maximum(count, capped)

    for k in range(NZ):
        back_out[k] = balanced[k : k + 1]

    def send_back(k, carry):
        remote(back_out.at[k], back_mid.at[k], bz_send, bz_recv, along_z(-k)).start()
        return carry

    lax.fori_loop(1, NZ, send_back, 0)
    settle(back_mid.at[pl.ds(1, NZ - 1)], bz_recv)
    back_tile[...] = jnp.concatenate(
        [back_out[0]] + [back_mid[k] for k in range(1, NZ)], axis=0
    )

    def send_tile(j, carry):
        remote(back_tile, back_in.at[j], bt_send, bt_recv, in_plane_back(j)).start()
        return carry

    lax.fori_loop(1, PLANE, send_tile, 0)
    spot = jnp.where(
        lax.broadcasted_iota(i32, (ROW, pairs), 0) == lane, 1.0, 0.0
    ).astype(bf16)
    settle(back_in.at[pl.ds(1, PLANE - 1)], bt_recv)
    given = back_tile[...]
    for j in range(1, PLANE):
        given = jnp.where(group == j, back_in[j], given)
    high = given.astype(bf16)
    rest = given - high.astype(f32)
    middle = rest.astype(bf16)
    low = (rest - middle.astype(f32)).astype(bf16)
    parts = jnp.concatenate(
        [high.astype(f32), middle.astype(f32), low.astype(f32)], axis=0
    ).astype(bf16)
    looked = jnp.dot(parts, spot, preferred_element_type=f32)
    looked = (looked[0:NZ] + looked[NZ : 2 * NZ]) + looked[2 * NZ : 3 * NZ]
    at_block = lax.broadcasted_iota(i32, (NZ, pairs), 0)
    out_ref[...] = jnp.sum(jnp.where(at_block == to_z, looked, 0.0), axis=0, keepdims=True)

    settle(meta_out.at[pl.ds(1, NZ - 1)], mz_send)
    settle(sent.at[pl.ds(1, NZ - 1)], z_send)
    settle(landed.at[:, pl.ds(1, PLANE - 1)], xy_send)
    settle(meta_in.at[pl.ds(1, PLANE - 1)], mt_send)
    settle(part_in.at[pl.ds(1, 3)], part_send)
    settle(back_out.at[pl.ds(1, NZ - 1)], bz_send)
    settle(back_in.at[pl.ds(1, PLANE - 1)], bt_send)


def body(text, concept_table, ids):
    pairs, quarter = text.shape
    held = concept_table.shape[0]
    f32, bf16 = jnp.float32, jnp.bfloat16
    vmem, dma = pltpu.VMEM, pltpu.SemaphoreType.DMA
    blocks = (NZ, PLANE, SLOT, quarter)
    out = pl.pallas_call(
        kernel,
        name="curate",
        out_shape=jax.ShapeDtypeStruct((1, pairs), f32),
        in_specs=[
            pl.BlockSpec(memory_space=pl.ANY),
            pl.BlockSpec(memory_space=pl.ANY),
            pl.BlockSpec(memory_space=pltpu.VMEM),
        ],
        out_specs=pl.BlockSpec(memory_space=pltpu.VMEM),
        scratch_shapes=[
            vmem((pairs, quarter), bf16),
            vmem((held, quarter), bf16),
            vmem((NZ, ROW, pairs), bf16),
            vmem(blocks, bf16),
            vmem(blocks, bf16),
            vmem(blocks, bf16),
            vmem((NZ, 1, ROW), f32),
            vmem((NZ, 1, ROW), f32),
            vmem((NZ, ROW), f32),
            vmem((PLANE, NZ, ROW), f32),
            vmem((NZ, ROW, ROW), f32),
            vmem((ROW, held), bf16),
            vmem((NZ, ROW, quarter), f32),
            vmem((3 * NZ, ROW), f32),
            vmem((4, 3 * NZ, ROW), f32),
            vmem((NZ, 1, ROW), f32),
            vmem((NZ, 1, ROW), f32),
            vmem((NZ, ROW), f32),
            vmem((PLANE, NZ, ROW), f32),
            dma((2,)),
            dma, dma((NZ,)), dma, dma, dma, dma,
            dma, dma((NZ,)), dma, dma, dma, dma, dma, dma,
        ],
        compiler_params=pltpu.CompilerParams(collective_id=0, has_side_effects=True),
    )(text, concept_table, ids.reshape(1, pairs))
    return out.reshape(pairs)


def solution(mesh):
    placed = (P("dp", "concept"), P("dp", "concept"), P("dp"))
    return jax.shard_map(body, mesh=mesh, in_specs=placed, out_specs=P("dp"), check_vma=False)
```

```python
import functools

import jax
import jax.numpy as jnp
from jax import lax
from jax.experimental import pallas as pl
from jax.experimental.pallas import tpu as pltpu
from jax.sharding import PartitionSpec as P

CAP = 16
SLOT = 8
NX, NZ, NY = 4, 8, 4
PLANE = NX * NY
ROW = PLANE * SLOT
Z_ORDER = (4, 3, 5, 2, 6, 1, 7)
PACKED = 88
MARK = 8192.0

logit_scale = 64.0
epsilon = 1e-06
f32, bf16, i32 = jnp.float32, jnp.bfloat16, jnp.int32


def one_hot(test):
    return jnp.where(test, 1.0, 0.0).astype(bf16)


def thirds(x):
    high = x.astype(bf16).astype(f32)
    middle = (x - high).astype(bf16).astype(f32)
    low = x - high - middle
    return [high, middle, low]


def down(square):
    filler = jnp.zeros((ROW - square.shape[0], ROW), f32)
    return jnp.transpose(jnp.concatenate([square, filler], axis=0))


def kernel(
    packed, text_hbm, table_hbm, ids_hbm, out_ref, flag_ref,
    ids_ref, text_v, table_v, kept, sent, carried, spread, spreaders, landed,
    meta_out, meta_mid, meta_tile, meta_in, ids_wide, hot, pieces,
    early_out, early_in, early_sum, early_far, early_half, early_other,
    part_out, part_in, back_out, back_mid, back_tile, back_in,
    load_sem, z_send, z_recv, mz_send, mz_recv, mt_send, mt_recv, xy_send, xy_recv,
    e_send, e_recv, part_send, part_recv, bz_send, bz_recv, bt_send, bt_recv,
):
    pairs = ids_ref.shape[1]
    held = table_v.shape[0]
    rows = packed or ROW
    me = lax.axis_index("dp")
    mine = lax.axis_index("concept")
    my_x, my_z, my_y = lax.div(me, NZ * NY), lax.rem(lax.div(me, NY), NZ), lax.rem(me, NY)
    core = lax.rem(mine, 2)
    far = lax.rem(mine + 2, 4)
    partner = mine + 1 - 2 * core
    across = lax.rem(partner + 2, 4)

    z_peer = [(me + (lax.rem(my_z + k, NZ) - my_z) * NY, mine) for k in range(NZ)]
    x_step = [(lax.rem(my_x + d, NX) - my_x) * (NZ * NY) for d in range(NX)]
    y_step = [lax.rem(my_y + d, NY) - my_y for d in range(NY)]
    peer = [(me + x_step[j // NY] + y_step[j % NY], mine) for j in range(PLANE)]
    peer_back = [peer[(-(j // NY)) % NX * NY + (-j) % NY] for j in range(PLANE)]
    concept_peer = [None, (me, partner), (me, far), (me, across)]

    def remote(src, dst, send, recv, device):
        return pltpu.make_async_remote_copy(
            src_ref=src, dst_ref=dst, send_sem=send, recv_sem=recv,
            device_id=device, device_id_type=pl.DeviceIdType.MESH,
        )

    def settle(ref, sem):
        pltpu.make_async_copy(ref, ref, sem).wait()

    barrier = pltpu.get_barrier_semaphore()

    def greet(device):
        pl.semaphore_signal(
            barrier, inc=1, device_id=device, device_id_type=pl.DeviceIdType.MESH
        )

    load_text = pltpu.make_async_copy(text_hbm, text_v, load_sem.at[0])
    load_ids = pltpu.make_async_copy(ids_hbm, ids_ref, load_sem.at[2])
    load_ids.start()
    for c in (2, 3):
        greet(concept_peer[c])
    for k in Z_ORDER:
        greet(z_peer[k])
    for j in range(1, PLANE):
        greet(peer[j])
    greet(concept_peer[1])
    load_text.start()
    load_table = pltpu.make_async_copy(table_hbm, table_v, load_sem.at[1])
    load_table.start()

    load_ids.wait()
    ids = ids_ref[...]
    owner = ((ids >> 10) * 43691) >> 17
    local = ids - owner * held
    to_z = (((owner >> 2) & 7) - my_z) & 7
    to_plane = ((((owner >> 5) - my_x) & 3) << 2) | (((owner & 3) - my_y) & 3)
    relative = to_z * PLANE + to_plane
    owners = lax.broadcasted_iota(i32, (NZ * PLANE, pairs), 0)
    is_owner = jnp.where(owners == relative, 1.0, 0.0)
    earlier = one_hot(
        lax.broadcasted_iota(i32, (pairs, pairs), 0)
        < lax.broadcasted_iota(i32, (pairs, pairs), 1)
    )
    is_owner_low = is_owner.astype(bf16)
    ahead = jnp.dot(is_owner_low, earlier, preferred_element_type=f32)
    rank = jnp.sum(is_owner * ahead, axis=0, keepdims=True).astype(i32)
    lane = to_plane * SLOT + rank
    target = to_z * ROW + lane
    mark = 0.0
    if packed:
        down_i = lax.broadcasted_iota(i32, (NZ * PLANE, NZ * PLANE), 0)
        over_i = lax.broadcasted_iota(i32, (NZ * PLANE, NZ * PLANE), 1)
        before = one_hot((over_i < down_i) & ((over_i >> 4) == (down_i >> 4)))
        held_by = jnp.sum(is_owner, axis=1, keepdims=True)
        held_by = jnp.broadcast_to(held_by, (NZ * PLANE, ROW)).astype(bf16)
        base = jnp.dot(before, held_by, preferred_element_type=f32)[:, 0:1]
        place = rank + jnp.sum(is_owner * base, axis=0, keepdims=True).astype(i32)
        full = jnp.max(place.astype(f32), axis=1, keepdims=True)
        mark = jnp.where(full >= float(packed), MARK, 0.0)
        place = to_z * ROW + place

    load_text.wait()
    ones = jnp.ones((SLOT, text_v.shape[1]), bf16)
    words = text_v[...].astype(f32)
    squares = words * words
    squares_high = squares.astype(bf16)
    squares_low = (squares - squares_high.astype(f32)).astype(bf16)
    across_lanes = (((1,), (1,)), ((), ()))
    tsq_pair = lax.dot_general(
        ones, squares_high, across_lanes, preferred_element_type=f32
    ) + lax.dot_general(ones, squares_low, across_lanes, preferred_element_type=f32)
    values = jnp.concatenate(
        [
            (local >> 6).astype(f32),
            (local & 63).astype(f32),
            jnp.ones((1, pairs), f32),
            *thirds(tsq_pair[0:1]),
            jnp.zeros((2, pairs), f32),
        ],
        axis=0,
    ).astype(bf16)
    slots = lax.broadcasted_iota(i32, (ROW, pairs), 0)
    for k in range(NZ):
        pick = one_hot(slots + k * ROW == target)
        meta = lax.dot_general(values, pick, across_lanes, preferred_element_type=f32)
        meta_out[k] = jnp.concatenate(
            [
                meta[0:1] * 64.0 + meta[1:2] + meta[2:3] - 1.0 + mark,
                (meta[3:4] + meta[4:5]) + meta[5:6],
            ],
            axis=0,
        )
        if k == 0:
            block = jnp.dot(pick, text_v[...], preferred_element_type=f32)
            kept[...] = block.reshape(PLANE, SLOT, -1).astype(bf16)

    pl.semaphore_wait(barrier, NZ - 1 + PLANE - 1 + 3)

    for k in Z_ORDER:
        remote(meta_out.at[k], meta_mid.at[k], mz_send, mz_recv, z_peer[k]).start()
    for k in Z_ORDER:
        if packed:
            pick = one_hot(slots[0:packed] + k * ROW == place)
        else:
            pick = one_hot(slots + k * ROW == target)
        block = jnp.dot(pick, text_v[...], preferred_element_type=f32)
        sent[k] = block.astype(bf16).reshape(sent.shape[1:])
        remote(sent.at[k], carried.at[k], z_send, z_recv.at[k], z_peer[k]).start()

    def pass_on(source, k):
        for j in range(1, PLANE):
            remote(source.at[j], landed.at[k, j], xy_send, xy_recv.at[k], peer[j]).start()

    pass_on(kept, 0)

    settle(meta_mid.at[pl.ds(1, NZ - 1)], mz_recv)
    metas = [meta_out[0]] + [meta_mid[k] for k in range(1, NZ)]
    tile = jnp.concatenate([m[0:1] for m in metas] + [m[1:2] for m in metas], axis=0)
    if packed:
        taken = tile[0:NZ] >= 0.0
        over = one_hot(
            lax.broadcasted_iota(i32, (ROW, ROW), 0) < lax.broadcasted_iota(i32, (ROW, ROW), 1)
        )
        spot = jnp.dot(one_hot(taken), over, preferred_element_type=f32)
        tile = jnp.concatenate([tile, jnp.where(taken, spot, -1.0)], axis=0)
    turned = down(tile)
    meta_tile[...] = turned.reshape(PLANE, SLOT, ROW)
    for j in range(1, PLANE):
        remote(meta_tile.at[j], meta_in.at[j], mt_send, mt_recv, peer[j]).start()
    if packed:
        lanes = lax.broadcasted_iota(i32, (ROW, packed), 1).astype(f32)
        for k in range(1, NZ):
            at = 2 * NZ + k
            spreaders[k] = one_hot(turned[:, at : at + 1] == lanes)

    def expand_and_pass(k):
        settle(carried.at[k], z_recv.at[k])
        if packed:
            block = jnp.dot(spreaders[k], carried[k], preferred_element_type=f32)
            spread[k] = block.reshape(PLANE, SLOT, -1).astype(bf16)
            pass_on(spread.at[k], k)
        else:
            pass_on(carried.at[k], k)

    expand_and_pass(Z_ORDER[0])

    settle(meta_in.at[pl.ds(1, PLANE - 1)], mt_recv)
    theirs = jnp.concatenate([meta_tile[0:1], meta_in[1:PLANE]], axis=0).reshape(ROW, ROW)
    by_row = jnp.transpose(theirs)
    slot_ids, tsq_part = by_row[0:NZ], by_row[NZ : 2 * NZ]
    flag_ref[0] = jnp.where(jnp.max(slot_ids) >= MARK * 0.5, 1, 0)
    for k in range(NZ):
        ids_wide[k] = jnp.broadcast_to(theirs[:, k : k + 1], (ROW, ROW))

    load_table.wait()
    columns = lax.broadcasted_iota(i32, (ROW, ROW), 1)
    columns_f = columns.astype(f32)

    def fetch(k, csq_cols):
        wanted = ids_wide[k]
        for c in range(held // ROW):
            hot[:, c * ROW : (c + 1) * ROW] = one_hot(wanted - float(c * ROW) == columns_f)
        piece = jnp.dot(hot[...], table_v[...], preferred_element_type=f32)
        pieces[k] = piece
        return jnp.where(columns == k, jnp.sum(piece * piece, axis=1, keepdims=True), csq_cols)

    csq_cols = jnp.zeros((ROW, ROW), f32)
    for step in range(4):
        csq_cols = lax.fori_loop(2 * step, 2 * step + 2, fetch, csq_cols)
        if step < 3:
            expand_and_pass(Z_ORDER[1 + step])
    early_out[0] = tsq_part
    early_out[1] = jnp.transpose(csq_cols)[0:NZ]

    remote(early_out, early_in, e_send.at[0], e_recv.at[0], concept_peer[1]).start()
    for k in Z_ORDER[4:6]:
        expand_and_pass(k)
    settle(early_in, e_recv.at[0])
    early_sum[...] = early_out[...] + early_in[...]
    remote(early_sum.at[core], early_far, e_send.at[1], e_recv.at[1], concept_peer[2]).start()
    expand_and_pass(Z_ORDER[6])

    dots = jnp.zeros((ROW, ROW), f32)
    for k in (0,) + Z_ORDER:
        settle(landed.at[k, pl.ds(1, PLANE - 1)], xy_recv.at[k])
        own = kept if k == 0 else spread.at[k] if packed else carried.at[k]
        words = jnp.concatenate(
            [own[0:1].astype(f32), landed[k, 1:PLANE].astype(f32)], axis=0
        ).reshape(ROW, -1)
        total = jnp.sum(words * pieces[k], axis=1, keepdims=True)
        dots = jnp.where(columns == k, total, dots)
    part_out[...] = jnp.transpose(dots)[0:NZ]

    for c in (2, 3, 1):
        remote(part_out, part_in.at[c], part_send, part_recv, concept_peer[c]).start()
    settle(early_far, e_recv.at[1])
    early_half[...] = early_sum[core] + early_far[...]
    remote(early_half, early_other, e_send.at[2], e_recv.at[2], concept_peer[1]).start()
    settle(early_other, e_recv.at[2])
    tsq = jnp.where(core == 0, early_half[...], early_other[...])
    csq = jnp.where(core == 0, early_other[...], early_half[...])
    inverse_t, inverse_c = lax.rsqrt(tsq + epsilon), lax.rsqrt(csq + epsilon)
    settle(part_in.at[pl.ds(1, 3)], part_recv)
    dot = (part_out[...] + part_in[1]) + (part_in[2] + part_in[3])
    match = jax.nn.sigmoid(logit_scale * dot * inverse_t * inverse_c)
    match = jnp.where(slot_ids >= 0.0, match, 0.0)

    match_turned = down(match)
    counts = [jnp.zeros((SLOT, ROW), f32) for _ in range(NZ)]
    for m in range(NZ):
        weight = jnp.broadcast_to(match_turned[:, m : m + 1], (ROW, ROW))
        theirs = ids_wide[m]
        for k in range(NZ):
            same = jnp.where(theirs == slot_ids[k : k + 1], weight, 0.0)
            counts[k] = counts[k] + jnp.sum(same.reshape(ROW // SLOT, SLOT, ROW), axis=0)
    count = jnp.concatenate([jnp.sum(c, axis=0, keepdims=True) for c in counts], axis=0)
    capped = CAP * 1.0
    balanced = match * capped / jnp.maximum(count, capped)

    for k in range(NZ):
        back_out[k] = balanced[k : k + 1]
    for k in Z_ORDER:
        remote(back_out.at[k], back_mid.at[k], bz_send, bz_recv, z_peer[NZ - k]).start()
    settle(back_mid.at[pl.ds(1, NZ - 1)], bz_recv)
    back_tile[...] = jnp.concatenate(
        [back_out[0]] + [back_mid[k] for k in range(1, NZ)], axis=0
    )
    for j in range(1, PLANE):
        remote(back_tile, back_in.at[j], bt_send, bt_recv, peer_back[j]).start()
    here = one_hot(slots == lane)
    settle(back_in.at[pl.ds(1, PLANE - 1)], bt_recv)
    group = lax.broadcasted_iota(i32, (NZ, ROW), 1) // SLOT
    given = back_tile[...]
    for j in range(1, PLANE):
        given = jnp.where(group == j, back_in[j], given)
    looked = jnp.dot(
        jnp.concatenate(thirds(given), axis=0).astype(bf16), here, preferred_element_type=f32
    )
    looked = (looked[0:NZ] + looked[NZ : 2 * NZ]) + looked[2 * NZ : 3 * NZ]
    at_block = lax.broadcasted_iota(i32, (NZ, pairs), 0)
    out_ref[...] = jnp.sum(jnp.where(at_block == to_z, looked, 0.0), axis=0, keepdims=True)

    settle(meta_out.at[pl.ds(1, NZ - 1)], mz_send)
    settle(sent.at[pl.ds(1, NZ - 1)], z_send)
    settle(landed.at[:, pl.ds(1, PLANE - 1)], xy_send)
    settle(meta_in.at[pl.ds(1, PLANE - 1)], mt_send)
    settle(early_out, e_send.at[0])
    settle(early_far, e_send.at[1])
    settle(early_half, e_send.at[2])
    settle(part_in.at[pl.ds(1, 3)], part_send)
    settle(back_out.at[pl.ds(1, NZ - 1)], bz_send)
    settle(back_in.at[pl.ds(1, PLANE - 1)], bt_send)


def curate(packed, text, concept_table, ids):
    pairs, quarter = text.shape
    held = concept_table.shape[0]
    vmem, dma = pltpu.VMEM, pltpu.SemaphoreType.DMA
    blocks = (NZ, PLANE, SLOT, quarter)
    moved = (NZ, packed, quarter) if packed else blocks
    return pl.pallas_call(
        functools.partial(kernel, packed),
        name="curate_packed" if packed else "curate_whole",
        out_shape=(
            jax.ShapeDtypeStruct((1, pairs), f32),
            jax.ShapeDtypeStruct((1,), i32),
        ),
        in_specs=[
            pl.BlockSpec(memory_space=pl.ANY),
            pl.BlockSpec(memory_space=pl.ANY),
            pl.BlockSpec(memory_space=pl.ANY),
        ],
        out_specs=(
            pl.BlockSpec(memory_space=pltpu.VMEM),
            pl.BlockSpec(memory_space=pltpu.SMEM),
        ),
        scratch_shapes=[
            vmem((1, pairs), i32),
            vmem((pairs, quarter), bf16),
            vmem((held, quarter), bf16),
            vmem((PLANE, SLOT, quarter), bf16),
            vmem(moved, bf16),
            vmem(moved, bf16),
            vmem(blocks if packed else (1, 1, SLOT, quarter), bf16),
            vmem((NZ, ROW, packed) if packed else (1, SLOT, ROW), bf16),
            vmem(blocks, bf16),
            vmem((NZ, 2, ROW), f32),
            vmem((NZ, 2, ROW), f32),
            vmem((PLANE, SLOT, ROW), f32),
            vmem((PLANE, SLOT, ROW), f32),
            vmem((NZ, ROW, ROW), f32),
            vmem((ROW, held), bf16),
            vmem((NZ, ROW, quarter), f32),
            vmem((2, NZ, ROW), f32),
            vmem((2, NZ, ROW), f32),
            vmem((2, NZ, ROW), f32),
            vmem((NZ, ROW), f32),
            vmem((NZ, ROW), f32),
            vmem((NZ, ROW), f32),
            vmem((NZ, ROW), f32),
            vmem((4, NZ, ROW), f32),
            vmem((NZ, 1, ROW), f32),
            vmem((NZ, 1, ROW), f32),
            vmem((NZ, ROW), f32),
            vmem((PLANE, NZ, ROW), f32),
            dma((3,)),
            dma, dma((NZ,)), dma, dma, dma, dma, dma, dma((NZ,)),
            dma((3,)), dma((3,)), dma, dma, dma, dma, dma, dma,
        ],
        compiler_params=pltpu.CompilerParams(
            collective_id=1 if packed else 0, has_side_effects=True
        ),
    )(text, concept_table, ids)


def body(text, concept_table, ids):
    pairs = text.shape[0]
    line = ids.reshape(1, pairs)
    out, over = curate(PACKED, text, concept_table, line)
    out = lax.cond(
        over[0] > 0,
        lambda: curate(0, text, concept_table, line)[0],
        lambda: out,
    )
    return out.reshape(pairs)


def solution(mesh):
    placed = (P("dp", "concept"), P("dp", "concept"), P("dp"))
    return jax.shard_map(body, mesh=mesh, in_specs=placed, out_specs=P("dp"), check_vma=False)
```

```python
import functools

import jax
import jax.numpy as jnp
from jax import lax
from jax.experimental import pallas as pl
from jax.experimental.pallas import tpu as pltpu
from jax.sharding import PartitionSpec as P

CAP = 16
SLOT = 8
NX, NZ, NY = 4, 8, 4
PLANE = NX * NY
ROW = PLANE * SLOT
Z_ORDER = (4, 3, 5, 2, 6, 1, 7)
PACKED = 88
MARK = 8192.0
HALF = NZ // 2

logit_scale = 64.0
epsilon = 1e-06
f32, bf16, i32 = jnp.float32, jnp.bfloat16, jnp.int32


def one_hot(test):
    return jnp.where(test, 1.0, 0.0).astype(bf16)


def thirds(x):
    high = x.astype(bf16).astype(f32)
    middle = (x - high).astype(bf16).astype(f32)
    low = x - high - middle
    return [high, middle, low]


def down(square):
    filler = jnp.zeros((ROW - square.shape[0], ROW), f32)
    return jnp.transpose(jnp.concatenate([square, filler], axis=0))


def kernel(
    packed, text_hbm, table_hbm, ids_hbm, out_ref, flag_ref,
    ids_ref, text_v, table_v, kept, sent, carried, spread, spreaders, landed,
    meta_out, meta_mid, meta_tile, meta_in, ids_wide, hot, pieces,
    early_out, early_in, early_sum, early_low, early_high, mid_wide,
    part_out, part_in, back_out, back_mid, back_tile, back_in,
    load_sem, z_send, z_recv, mz_send, mz_recv, mt_send, mt_recv, xy_send, xy_recv,
    e_send, e_recv, part_send, part_recv, bz_send, bz_recv, bt_send, bt_recv,
):
    pairs = ids_ref.shape[1]
    held = table_v.shape[0]
    rows = packed or ROW
    me = lax.axis_index("dp")
    mine = lax.axis_index("concept")
    my_x, my_z, my_y = lax.div(me, NZ * NY), lax.rem(lax.div(me, NY), NZ), lax.rem(me, NY)
    core = lax.rem(mine, 2)
    partner = mine + 1 - 2 * core
    my_ring = lax.div(mine, 2) * NZ + my_z

    z_peer = [(me + (lax.rem(my_z + k, NZ) - my_z) * NY, mine) for k in range(NZ)]
    x_step = [(lax.rem(my_x + d, NX) - my_x) * (NZ * NY) for d in range(NX)]
    y_step = [lax.rem(my_y + d, NY) - my_y for d in range(NY)]
    peer = [(me + x_step[j // NY] + y_step[j % NY], mine) for j in range(PLANE)]
    peer_back = [peer[(-(j // NY)) % NX * NY + (-j) % NY] for j in range(PLANE)]
    other_core = (me, partner)

    def ring(step, on_core):
        there = lax.rem(my_ring + step + 2 * NZ, 2 * NZ)
        return (me + (lax.rem(there, NZ) - my_z) * NY, lax.div(there, NZ) * 2 + on_core)

    nearby = {e: ring(e, core) for e in range(-HALF, HALF + 1)}

    def remote(src, dst, send, recv, device):
        return pltpu.make_async_remote_copy(
            src_ref=src, dst_ref=dst, send_sem=send, recv_sem=recv,
            device_id=device, device_id_type=pl.DeviceIdType.MESH,
        )

    def settle(ref, sem):
        pltpu.make_async_copy(ref, ref, sem).wait()

    barrier = pltpu.get_barrier_semaphore()

    def greet(device):
        pl.semaphore_signal(
            barrier, inc=1, device_id=device, device_id_type=pl.DeviceIdType.MESH
        )

    load_text = pltpu.make_async_copy(text_hbm, text_v, load_sem.at[0])
    load_ids = pltpu.make_async_copy(ids_hbm, ids_ref, load_sem.at[2])
    load_ids.start()
    for k in Z_ORDER:
        greet(z_peer[k])
    for j in range(1, PLANE):
        greet(peer[j])
    for e in range(1, HALF + 1):
        greet(nearby[e])
        greet(nearby[-e])
    greet(ring(HALF, 1 - core))
    greet(ring(-HALF, 1 - core))
    greet(other_core)
    load_text.start()
    load_table = pltpu.make_async_copy(table_hbm, table_v, load_sem.at[1])
    load_table.start()

    load_ids.wait()
    ids = ids_ref[...]
    owner = ((ids >> 10) * 43691) >> 17
    local = ids - owner * held
    to_z = (((owner >> 2) & 7) - my_z) & 7
    to_plane = ((((owner >> 5) - my_x) & 3) << 2) | (((owner & 3) - my_y) & 3)
    relative = to_z * PLANE + to_plane
    owners = lax.broadcasted_iota(i32, (NZ * PLANE, pairs), 0)
    is_owner = jnp.where(owners == relative, 1.0, 0.0)
    earlier = one_hot(
        lax.broadcasted_iota(i32, (pairs, pairs), 0)
        < lax.broadcasted_iota(i32, (pairs, pairs), 1)
    )
    is_owner_low = is_owner.astype(bf16)
    ahead = jnp.dot(is_owner_low, earlier, preferred_element_type=f32)
    rank = jnp.sum(is_owner * ahead, axis=0, keepdims=True).astype(i32)
    lane = to_plane * SLOT + rank
    target = to_z * ROW + lane
    mark = 0.0
    if packed:
        down_i = lax.broadcasted_iota(i32, (NZ * PLANE, NZ * PLANE), 0)
        over_i = lax.broadcasted_iota(i32, (NZ * PLANE, NZ * PLANE), 1)
        before = one_hot((over_i < down_i) & ((over_i >> 4) == (down_i >> 4)))
        held_by = jnp.sum(is_owner, axis=1, keepdims=True)
        held_by = jnp.broadcast_to(held_by, (NZ * PLANE, ROW)).astype(bf16)
        base = jnp.dot(before, held_by, preferred_element_type=f32)[:, 0:1]
        place = rank + jnp.sum(is_owner * base, axis=0, keepdims=True).astype(i32)
        full = jnp.max(place.astype(f32), axis=1, keepdims=True)
        mark = jnp.where(full >= float(packed), MARK, 0.0)
        place = to_z * ROW + place

    load_text.wait()
    ones = jnp.ones((SLOT, text_v.shape[1]), bf16)
    words = text_v[...].astype(f32)
    squares = words * words
    squares_high = squares.astype(bf16)
    squares_low = (squares - squares_high.astype(f32)).astype(bf16)
    across_lanes = (((1,), (1,)), ((), ()))
    tsq_pair = lax.dot_general(
        ones, squares_high, across_lanes, preferred_element_type=f32
    ) + lax.dot_general(ones, squares_low, across_lanes, preferred_element_type=f32)
    values = jnp.concatenate(
        [
            (local >> 6).astype(f32),
            (local & 63).astype(f32),
            jnp.ones((1, pairs), f32),
            *thirds(tsq_pair[0:1]),
            jnp.zeros((2, pairs), f32),
        ],
        axis=0,
    ).astype(bf16)
    slots = lax.broadcasted_iota(i32, (ROW, pairs), 0)
    for k in range(NZ):
        pick = one_hot(slots + k * ROW == target)
        meta = lax.dot_general(values, pick, across_lanes, preferred_element_type=f32)
        meta_out[k] = jnp.concatenate(
            [
                meta[0:1] * 64.0 + meta[1:2] + meta[2:3] - 1.0 + mark,
                (meta[3:4] + meta[4:5]) + meta[5:6],
            ],
            axis=0,
        )
        if k == 0:
            block = jnp.dot(pick, text_v[...], preferred_element_type=f32)
            kept[...] = block.reshape(PLANE, SLOT, -1).astype(bf16)

    pl.semaphore_wait(barrier, NZ - 1 + PLANE - 1 + 2 * HALF + 3)

    for k in Z_ORDER:
        remote(meta_out.at[k], meta_mid.at[k], mz_send, mz_recv, z_peer[k]).start()
    for k in Z_ORDER:
        if packed:
            pick = one_hot(slots[0:packed] + k * ROW == place)
        else:
            pick = one_hot(slots + k * ROW == target)
        block = jnp.dot(pick, text_v[...], preferred_element_type=f32)
        sent[k] = block.astype(bf16).reshape(sent.shape[1:])
        remote(sent.at[k], carried.at[k], z_send, z_recv.at[k], z_peer[k]).start()

    def pass_on(source, k):
        for j in range(1, PLANE):
            remote(source.at[j], landed.at[k, j], xy_send, xy_recv.at[k], peer[j]).start()

    pass_on(kept, 0)

    settle(meta_mid.at[pl.ds(1, NZ - 1)], mz_recv)
    metas = [meta_out[0]] + [meta_mid[k] for k in range(1, NZ)]
    tile = jnp.concatenate([m[0:1] for m in metas] + [m[1:2] for m in metas], axis=0)
    if packed:
        taken = tile[0:NZ] >= 0.0
        over = one_hot(
            lax.broadcasted_iota(i32, (ROW, ROW), 0) < lax.broadcasted_iota(i32, (ROW, ROW), 1)
        )
        spot = jnp.dot(one_hot(taken), over, preferred_element_type=f32)
        tile = jnp.concatenate([tile, jnp.where(taken, spot, -1.0)], axis=0)
    turned = down(tile)
    meta_tile[...] = turned.reshape(PLANE, SLOT, ROW)
    for j in range(1, PLANE):
        remote(meta_tile.at[j], meta_in.at[j], mt_send, mt_recv, peer[j]).start()
    if packed:
        lanes = lax.broadcasted_iota(i32, (ROW, packed), 1).astype(f32)
        for k in range(1, NZ):
            at = 2 * NZ + k
            spreaders[k] = one_hot(turned[:, at : at + 1] == lanes)

    def expand_and_pass(k):
        settle(carried.at[k], z_recv.at[k])
        if packed:
            block = jnp.dot(spreaders[k], carried[k], preferred_element_type=f32)
            spread[k] = block.reshape(PLANE, SLOT, -1).astype(bf16)
            pass_on(spread.at[k], k)
        else:
            pass_on(carried.at[k], k)

    expand_and_pass(Z_ORDER[0])

    settle(meta_in.at[pl.ds(1, PLANE - 1)], mt_recv)
    theirs = jnp.concatenate([meta_tile[0:1], meta_in[1:PLANE]], axis=0).reshape(ROW, ROW)
    by_row = jnp.transpose(theirs)
    slot_ids, tsq_part = by_row[0:NZ], by_row[NZ : 2 * NZ]
    flag_ref[0] = jnp.where(jnp.max(slot_ids) >= MARK * 0.5, 1, 0)
    for k in range(NZ):
        ids_wide[k] = jnp.broadcast_to(theirs[:, k : k + 1], (ROW, ROW))

    load_table.wait()
    columns = lax.broadcasted_iota(i32, (ROW, ROW), 1)
    columns_f = columns.astype(f32)

    def fetch(k, csq_cols):
        wanted = ids_wide[k]
        for c in range(held // ROW):
            hot[:, c * ROW : (c + 1) * ROW] = one_hot(wanted - float(c * ROW) == columns_f)
        piece = jnp.dot(hot[...], table_v[...], preferred_element_type=f32)
        pieces[k] = piece
        return jnp.where(columns == k, jnp.sum(piece * piece, axis=1, keepdims=True), csq_cols)

    csq_cols = jnp.zeros((ROW, ROW), f32)
    for step in range(4):
        csq_cols = lax.fori_loop(2 * step, 2 * step + 2, fetch, csq_cols)
        if step < 3:
            expand_and_pass(Z_ORDER[1 + step])
    early_out[0] = tsq_part
    early_out[1] = jnp.transpose(csq_cols)[0:NZ]

    remote(early_out, early_in, e_send.at[0], e_recv.at[0], other_core).start()
    for k in Z_ORDER[4:6]:
        expand_and_pass(k)
    settle(early_in, e_recv.at[0])
    early_sum[0] = early_out[0] + early_in[0]
    early_sum[1] = early_out[1] + early_in[1]
    early_sum[2] = slot_ids
    remote(early_sum, early_low, e_send.at[1], e_recv.at[1], nearby[HALF]).start()
    remote(
        early_sum.at[pl.ds(0, 2)], early_high, e_send.at[2], e_recv.at[2], nearby[-HALF]
    ).start()
    expand_and_pass(Z_ORDER[6])

    dots = jnp.zeros((ROW, ROW), f32)
    for k in (0,) + Z_ORDER:
        settle(landed.at[k, pl.ds(1, PLANE - 1)], xy_recv.at[k])
        own = kept if k == 0 else spread.at[k] if packed else carried.at[k]
        words = jnp.concatenate(
            [own[0:1].astype(f32), landed[k, 1:PLANE].astype(f32)], axis=0
        ).reshape(ROW, -1)
        total = jnp.sum(words * pieces[k], axis=1, keepdims=True)
        dots = jnp.where(columns == k, total, dots)
    part_out[...] = jnp.transpose(dots)[0:NZ]

    for c in (core, 1 - core):
        remote(part_out, part_in.at[core], part_send, part_recv, ring(HALF, c)).start()
        remote(part_out, part_in.at[2 + core], part_send, part_recv, ring(-HALF, c)).start()
    settle(early_low, e_recv.at[1])
    settle(early_high, e_recv.at[2])
    inverse_t = lax.rsqrt(early_low[0] + early_high[0] + epsilon)
    inverse_c = lax.rsqrt(early_low[1] + early_high[1] + epsilon)
    mid_ids = early_low[2]
    turned = down(mid_ids)
    for k in range(NZ):
        mid_wide[k] = jnp.broadcast_to(turned[:, k : k + 1], (ROW, ROW))
    settle(part_in, part_recv)
    dot = (part_in[0] + part_in[1]) + (part_in[2] + part_in[3])
    match = jax.nn.sigmoid(logit_scale * dot * inverse_t * inverse_c)
    match = jnp.where(mid_ids >= 0.0, match, 0.0)

    match_turned = down(match)
    counts = [jnp.zeros((SLOT, ROW), f32) for _ in range(NZ)]
    for m in range(NZ):
        weight = jnp.broadcast_to(match_turned[:, m : m + 1], (ROW, ROW))
        theirs = mid_wide[m]
        for k in range(NZ):
            same = jnp.where(theirs == mid_ids[k : k + 1], weight, 0.0)
            counts[k] = counts[k] + jnp.sum(same.reshape(ROW // SLOT, SLOT, ROW), axis=0)
    count = jnp.concatenate([jnp.sum(c, axis=0, keepdims=True) for c in counts], axis=0)
    capped = CAP * 1.0
    balanced = match * capped / jnp.maximum(count, capped)

    for k in range(NZ):
        back_out[(k + HALF) % NZ] = balanced[k : k + 1]
    for k in (0, 7, 1, 6, 2, 5, 3):
        i = (k + HALF) % NZ
        remote(back_out.at[i], back_mid.at[i], bz_send, bz_recv, nearby[HALF - k]).start()
    settle(back_mid.at[pl.ds(1, NZ - 1)], bz_recv)
    back_tile[...] = jnp.concatenate(
        [back_out[0] if k == HALF else back_mid[(k + HALF) % NZ] for k in range(NZ)], axis=0
    )
    for j in range(1, PLANE):
        remote(back_tile, back_in.at[j], bt_send, bt_recv, peer_back[j]).start()
    here = one_hot(slots == lane)
    settle(back_in.at[pl.ds(1, PLANE - 1)], bt_recv)
    group = lax.broadcasted_iota(i32, (NZ, ROW), 1) // SLOT
    given = back_tile[...]
    for j in range(1, PLANE):
        given = jnp.where(group == j, back_in[j], given)
    looked = jnp.dot(
        jnp.concatenate(thirds(given), axis=0).astype(bf16), here, preferred_element_type=f32
    )
    looked = (looked[0:NZ] + looked[NZ : 2 * NZ]) + looked[2 * NZ : 3 * NZ]
    at_block = lax.broadcasted_iota(i32, (NZ, pairs), 0)
    out_ref[...] = jnp.sum(jnp.where(at_block == to_z, looked, 0.0), axis=0, keepdims=True)

    settle(meta_out.at[pl.ds(1, NZ - 1)], mz_send)
    settle(sent.at[pl.ds(1, NZ - 1)], z_send)
    settle(landed.at[:, pl.ds(1, PLANE - 1)], xy_send)
    settle(meta_in.at[pl.ds(1, PLANE - 1)], mt_send)
    settle(early_out, e_send.at[0])
    settle(early_low, e_send.at[1])
    settle(early_high, e_send.at[2])
    settle(part_in, part_send)
    settle(back_out.at[pl.ds(1, NZ - 1)], bz_send)
    settle(back_in.at[pl.ds(1, PLANE - 1)], bt_send)


def curate(packed, text, concept_table, ids):
    pairs, quarter = text.shape
    held = concept_table.shape[0]
    vmem, dma = pltpu.VMEM, pltpu.SemaphoreType.DMA
    blocks = (NZ, PLANE, SLOT, quarter)
    moved = (NZ, packed, quarter) if packed else blocks
    return pl.pallas_call(
        functools.partial(kernel, packed),
        name="curate_packed" if packed else "curate_whole",
        out_shape=(
            jax.ShapeDtypeStruct((1, pairs), f32),
            jax.ShapeDtypeStruct((1,), i32),
        ),
        in_specs=[
            pl.BlockSpec(memory_space=pl.ANY),
            pl.BlockSpec(memory_space=pl.ANY),
            pl.BlockSpec(memory_space=pl.ANY),
        ],
        out_specs=(
            pl.BlockSpec(memory_space=pltpu.VMEM),
            pl.BlockSpec(memory_space=pltpu.SMEM),
        ),
        scratch_shapes=[
            vmem((1, pairs), i32),
            vmem((pairs, quarter), bf16),
            vmem((held, quarter), bf16),
            vmem((PLANE, SLOT, quarter), bf16),
            vmem(moved, bf16),
            vmem(moved, bf16),
            vmem(blocks if packed else (1, 1, SLOT, quarter), bf16),
            vmem((NZ, ROW, packed) if packed else (1, SLOT, ROW), bf16),
            vmem(blocks, bf16),
            vmem((NZ, 2, ROW), f32),
            vmem((NZ, 2, ROW), f32),
            vmem((PLANE, SLOT, ROW), f32),
            vmem((PLANE, SLOT, ROW), f32),
            vmem((NZ, ROW, ROW), f32),
            vmem((ROW, held), bf16),
            vmem((NZ, ROW, quarter), f32),
            vmem((2, NZ, ROW), f32),
            vmem((2, NZ, ROW), f32),
            vmem((3, NZ, ROW), f32),
            vmem((3, NZ, ROW), f32),
            vmem((2, NZ, ROW), f32),
            vmem((NZ, ROW, ROW), f32),
            vmem((NZ, ROW), f32),
            vmem((4, NZ, ROW), f32),
            vmem((NZ, 1, ROW), f32),
            vmem((NZ, 1, ROW), f32),
            vmem((NZ, ROW), f32),
            vmem((PLANE, NZ, ROW), f32),
            dma((3,)),
            dma, dma((NZ,)), dma, dma, dma, dma, dma, dma((NZ,)),
            dma((3,)), dma((3,)), dma, dma, dma, dma, dma, dma,
        ],
        compiler_params=pltpu.CompilerParams(
            collective_id=1 if packed else 0, has_side_effects=True
        ),
    )(text, concept_table, ids)


def body(text, concept_table, ids):
    pairs = text.shape[0]
    line = ids.reshape(1, pairs)
    out, over = curate(PACKED, text, concept_table, line)
    out = lax.cond(
        over[0] > 0,
        lambda: curate(0, text, concept_table, line)[0],
        lambda: out,
    )
    return out.reshape(pairs)


def solution(mesh):
    placed = (P("dp", "concept"), P("dp", "concept"), P("dp"))
    return jax.shard_map(body, mesh=mesh, in_specs=placed, out_specs=P("dp"), check_vma=False)
```

```python
import functools

import jax
import jax.numpy as jnp
from jax import lax
from jax.experimental import pallas as pl
from jax.experimental.pallas import tpu as pltpu
from jax.sharding import PartitionSpec as P

CAP = 16
SLOT = 8
NX, NZ, NY = 4, 8, 4
PLANE = NX * NY
ROW = PLANE * SLOT
Z_ORDER = (4, 3, 5, 2, 6, 1, 7)
Z_FIRST = (4, 3, 5)
PLANE_FIRST = (2, 6, 1, 7)
PACKED = 88
PACKED_LATE = 96
MARK = 8192.0
HALF = NZ // 2

logit_scale = 64.0
epsilon = 1e-06
f32, bf16, i32 = jnp.float32, jnp.bfloat16, jnp.int32


def one_hot(test):
    return jnp.where(test, 1.0, 0.0).astype(bf16)


def thirds(x):
    high = x.astype(bf16).astype(f32)
    middle = (x - high).astype(bf16).astype(f32)
    low = x - high - middle
    return [high, middle, low]


def down(square):
    filler = jnp.zeros((ROW - square.shape[0], ROW), f32)
    return jnp.transpose(jnp.concatenate([square, filler], axis=0))


def kernel(
    packed, text_hbm, table_hbm, ids_hbm, out_ref, flag_ref,
    ids_ref, text_v, table_v, kept, sent, carried, spread, spreaders, landed,
    late_sent, late_carried, late_spreaders, taken_out, taken_in,
    meta_out, meta_mid, meta_tile, meta_in, ids_wide, hot, pieces,
    early_out, early_in, early_sum, early_low, early_high, mid_wide,
    part_out, part_in, back_out, back_mid, back_tile, back_in,
    load_sem, z_send, z_recv, mz_send, mz_recv, mt_send, mt_recv, xy_send, xy_recv,
    e_send, e_recv, part_send, part_recv, bz_send, bz_recv, bt_send, bt_recv,
    late_send, taken_send, taken_recv,
):
    pairs = ids_ref.shape[1]
    held = table_v.shape[0]
    first = Z_FIRST if packed else Z_ORDER
    late = PLANE_FIRST if packed else ()
    me = lax.axis_index("dp")
    mine = lax.axis_index("concept")
    my_x, my_z, my_y = lax.div(me, NZ * NY), lax.rem(lax.div(me, NY), NZ), lax.rem(me, NY)
    core = lax.rem(mine, 2)
    partner = mine + 1 - 2 * core
    my_ring = lax.div(mine, 2) * NZ + my_z

    z_peer = [(me + (lax.rem(my_z + k, NZ) - my_z) * NY, mine) for k in range(NZ)]
    x_step = [(lax.rem(my_x + d, NX) - my_x) * (NZ * NY) for d in range(NX)]
    y_step = [lax.rem(my_y + d, NY) - my_y for d in range(NY)]
    peer = [(me + x_step[j // NY] + y_step[j % NY], mine) for j in range(PLANE)]
    peer_back = [peer[(-(j // NY)) % NX * NY + (-j) % NY] for j in range(PLANE)]
    other_core = (me, partner)

    def ring(step, on_core):
        there = lax.rem(my_ring + step + 2 * NZ, 2 * NZ)
        return (me + (lax.rem(there, NZ) - my_z) * NY, lax.div(there, NZ) * 2 + on_core)

    nearby = {e: ring(e, core) for e in range(-HALF, HALF + 1)}

    def remote(src, dst, send, recv, device):
        return pltpu.make_async_remote_copy(
            src_ref=src, dst_ref=dst, send_sem=send, recv_sem=recv,
            device_id=device, device_id_type=pl.DeviceIdType.MESH,
        )

    def settle(ref, sem):
        pltpu.make_async_copy(ref, ref, sem).wait()

    barrier = pltpu.get_barrier_semaphore()

    def greet(device):
        pl.semaphore_signal(
            barrier, inc=1, device_id=device, device_id_type=pl.DeviceIdType.MESH
        )

    load_text = pltpu.make_async_copy(text_hbm, text_v, load_sem.at[0])
    load_ids = pltpu.make_async_copy(ids_hbm, ids_ref, load_sem.at[2])
    load_ids.start()
    for k in Z_ORDER:
        greet(z_peer[k])
    for j in range(1, PLANE):
        greet(peer[j])
    for e in range(1, HALF + 1):
        greet(nearby[e])
        greet(nearby[-e])
    greet(ring(HALF, 1 - core))
    greet(ring(-HALF, 1 - core))
    greet(other_core)
    load_text.start()
    load_table = pltpu.make_async_copy(table_hbm, table_v, load_sem.at[1])
    load_table.start()

    load_ids.wait()
    ids = ids_ref[...]
    owner = ((ids >> 10) * 43691) >> 17
    local = ids - owner * held
    to_z = (((owner >> 2) & 7) - my_z) & 7
    to_plane = ((((owner >> 5) - my_x) & 3) << 2) | (((owner & 3) - my_y) & 3)
    relative = to_z * PLANE + to_plane
    owners = lax.broadcasted_iota(i32, (NZ * PLANE, pairs), 0)
    is_owner = jnp.where(owners == relative, 1.0, 0.0)
    earlier = one_hot(
        lax.broadcasted_iota(i32, (pairs, pairs), 0)
        < lax.broadcasted_iota(i32, (pairs, pairs), 1)
    )
    is_owner_low = is_owner.astype(bf16)
    ahead = jnp.dot(is_owner_low, earlier, preferred_element_type=f32)
    rank = jnp.sum(is_owner * ahead, axis=0, keepdims=True).astype(i32)
    lane = to_plane * SLOT + rank
    target = to_z * ROW + lane
    mark = 0.0
    if packed:
        down_i = lax.broadcasted_iota(i32, (NZ * PLANE, NZ * PLANE), 0)
        over_i = lax.broadcasted_iota(i32, (NZ * PLANE, NZ * PLANE), 1)
        before = one_hot((over_i < down_i) & ((over_i >> 4) == (down_i >> 4)))
        held_by = jnp.sum(is_owner, axis=1, keepdims=True)
        held_by = jnp.broadcast_to(held_by, (NZ * PLANE, ROW)).astype(bf16)
        base = jnp.dot(before, held_by, preferred_element_type=f32)[:, 0:1]
        place = rank + jnp.sum(is_owner * base, axis=0, keepdims=True).astype(i32)
        full = jnp.max(place.astype(f32), axis=1, keepdims=True)
        mark = jnp.where(full >= float(packed), MARK, 0.0)
        place = to_z * ROW + place

    load_text.wait()
    ones = jnp.ones((SLOT, text_v.shape[1]), bf16)
    words = text_v[...].astype(f32)
    squares = words * words
    squares_high = squares.astype(bf16)
    squares_low = (squares - squares_high.astype(f32)).astype(bf16)
    across_lanes = (((1,), (1,)), ((), ()))
    tsq_pair = lax.dot_general(
        ones, squares_high, across_lanes, preferred_element_type=f32
    ) + lax.dot_general(ones, squares_low, across_lanes, preferred_element_type=f32)
    values = jnp.concatenate(
        [
            (local >> 6).astype(f32),
            (local & 63).astype(f32),
            jnp.ones((1, pairs), f32),
            *thirds(tsq_pair[0:1]),
            jnp.zeros((2, pairs), f32),
        ],
        axis=0,
    ).astype(bf16)
    slots = lax.broadcasted_iota(i32, (ROW, pairs), 0)
    taken_rows = {}
    for k in range(NZ):
        pick = one_hot(slots + k * ROW == target)
        meta = lax.dot_general(values, pick, across_lanes, preferred_element_type=f32)
        meta_out[k] = jnp.concatenate(
            [
                meta[0:1] * 64.0 + meta[1:2] + meta[2:3] - 1.0 + mark,
                (meta[3:4] + meta[4:5]) + meta[5:6],
            ],
            axis=0,
        )
        taken_rows[k] = meta[2:3]
        if k == 0 or k in late:
            at = (late.index(k) + 1) if k else 0
            block = jnp.dot(pick, text_v[...], preferred_element_type=f32)
            kept[at] = block.reshape(PLANE, SLOT, -1).astype(bf16)
    if packed:
        filler = jnp.zeros((SLOT - len(late), ROW), f32)
        tile = jnp.concatenate([taken_rows[k] for k in late] + [filler], axis=0)
        taken_out[...] = down(tile).reshape(PLANE, SLOT, ROW).astype(bf16)

    pl.semaphore_wait(barrier, NZ - 1 + PLANE - 1 + 2 * HALF + 3)

    for k in Z_ORDER:
        remote(meta_out.at[k], meta_mid.at[k], mz_send, mz_recv, z_peer[k]).start()
    for i, k in enumerate(first):
        if packed:
            pick = one_hot(slots[0:packed] + k * ROW == place)
        else:
            pick = one_hot(slots + k * ROW == target)
        block = jnp.dot(pick, text_v[...], preferred_element_type=f32)
        sent[i] = block.astype(bf16).reshape(sent.shape[1:])
        remote(sent.at[i], carried.at[i], z_send, z_recv.at[k], z_peer[k]).start()

    def pass_on(source, k):
        for j in range(1, PLANE):
            remote(source.at[j], landed.at[k, j], xy_send, xy_recv.at[k], peer[j]).start()

    if packed:
        for j in range(1, PLANE):
            remote(taken_out.at[j], taken_in.at[j], taken_send, taken_recv, peer[j]).start()
    for i, k in enumerate(late):
        pass_on(kept.at[i + 1], k)
    pass_on(kept.at[0], 0)

    def arrived(k, own):
        settle(landed.at[k, pl.ds(1, PLANE - 1)], xy_recv.at[k])
        return jnp.concatenate(
            [own[0:1].astype(f32), landed[k, 1:PLANE].astype(f32)], axis=0
        ).reshape(ROW, -1)

    over = one_hot(
        lax.broadcasted_iota(i32, (ROW, ROW), 0) < lax.broadcasted_iota(i32, (ROW, ROW), 1)
    )

    def places(taken):
        spot = jnp.dot(one_hot(taken), over, preferred_element_type=f32)
        return jnp.where(taken, spot, -1.0)

    settle(meta_mid.at[pl.ds(1, NZ - 1)], mz_recv)
    metas = [meta_out[0]] + [meta_mid[k] for k in range(1, NZ)]
    tile = jnp.concatenate([m[0:1] for m in metas] + [m[1:2] for m in metas], axis=0)
    if packed:
        tile = jnp.concatenate([tile, places(tile[0:NZ] >= 0.0)], axis=0)
    turned = down(tile)
    meta_tile[...] = turned.reshape(PLANE, SLOT, ROW)
    for j in range(1, PLANE):
        remote(meta_tile.at[j], meta_in.at[j], mt_send, mt_recv, peer[j]).start()
    if packed:
        lanes = lax.broadcasted_iota(i32, (ROW, packed), 1).astype(f32)
        for i, k in enumerate(first):
            at = 2 * NZ + k
            spreaders[i] = one_hot(turned[:, at : at + 1] == lanes)

    def expand_and_pass(i):
        k = first[i]
        settle(carried.at[i], z_recv.at[k])
        if packed:
            block = jnp.dot(spreaders[i], carried[i], preferred_element_type=f32)
            spread[i] = block.reshape(PLANE, SLOT, -1).astype(bf16)
            pass_on(spread.at[i], k)
        else:
            pass_on(carried.at[i], k)

    if packed:
        settle(taken_in.at[pl.ds(1, PLANE - 1)], taken_recv)
        theirs = jnp.concatenate(
            [taken_out[0:1].astype(f32), taken_in[1:PLANE].astype(f32)], axis=0
        ).reshape(ROW, ROW)
        late_place = places(jnp.transpose(theirs)[0:NZ] > 0.5)
        late_rows = lax.broadcasted_iota(i32, (PACKED_LATE, ROW), 0).astype(f32)

    def pack_late(i):
        k = late[i]
        block = arrived(k, kept.at[i + 1]).astype(bf16)
        pick = one_hot(late_rows == late_place[i : i + 1])
        late_sent[i] = jnp.dot(pick, block, preferred_element_type=f32).astype(bf16)
        remote(late_sent.at[i], late_carried.at[i], late_send, z_recv.at[k], z_peer[k]).start()

    for i in range(len(late)):
        pack_late(i)
    expand_and_pass(0)

    settle(meta_in.at[pl.ds(1, PLANE - 1)], mt_recv)
    theirs = jnp.concatenate([meta_tile[0:1], meta_in[1:PLANE]], axis=0).reshape(ROW, ROW)
    by_row = jnp.transpose(theirs)
    slot_ids, tsq_part = by_row[0:NZ], by_row[NZ : 2 * NZ]
    bad = jnp.max(jnp.max(slot_ids, axis=1, keepdims=True), axis=0, keepdims=True) >= MARK * 0.5
    if packed:
        here = places(slot_ids >= 0.0)
        late_here = jnp.concatenate([here[k : k + 1] for k in late], axis=0)
        most = jnp.max(jnp.max(late_here, axis=1, keepdims=True), axis=0, keepdims=True)
        bad = bad | (most >= float(PACKED_LATE))
        turned = down(here)
        lanes = lax.broadcasted_iota(i32, (ROW, PACKED_LATE), 1).astype(f32)
        for i, k in enumerate(late):
            late_spreaders[i] = one_hot(turned[:, k : k + 1] == lanes)
    bad = jnp.where(bad, MARK, 0.0)
    for k in range(NZ):
        ids_wide[k] = jnp.broadcast_to(theirs[:, k : k + 1], (ROW, ROW))

    load_table.wait()
    columns = lax.broadcasted_iota(i32, (ROW, ROW), 1)
    columns_f = columns.astype(f32)

    def fetch(k, csq_cols):
        wanted = ids_wide[k]
        for c in range(held // ROW):
            hot[:, c * ROW : (c + 1) * ROW] = one_hot(wanted - float(c * ROW) == columns_f)
        piece = jnp.dot(hot[...], table_v[...], preferred_element_type=f32)
        pieces[k] = piece
        return jnp.where(columns == k, jnp.sum(piece * piece, axis=1, keepdims=True), csq_cols)

    csq_cols = jnp.zeros((ROW, ROW), f32)
    for step in range(4):
        csq_cols = lax.fori_loop(2 * step, 2 * step + 2, fetch, csq_cols)
        if 1 + step < len(first):
            expand_and_pass(1 + step)
    early_out[0] = tsq_part
    early_out[1] = jnp.transpose(csq_cols)[0:NZ]

    remote(early_out, early_in, e_send.at[0], e_recv.at[0], other_core).start()
    for i in range(5, len(first)):
        expand_and_pass(i)

    dots = jnp.zeros((ROW, ROW), f32)
    for k in (0,) + first + late:
        if k in late:
            i = late.index(k)
            settle(late_carried.at[i], z_recv.at[k])
            words = jnp.dot(late_spreaders[i], late_carried[i], preferred_element_type=f32)
        elif k == 0:
            words = arrived(k, kept.at[0])
        else:
            i = first.index(k)
            words = arrived(k, spread.at[i] if packed else carried.at[i])
        total = jnp.sum(words * pieces[k], axis=1, keepdims=True)
        dots = jnp.where(columns == k, total, dots)
        if k == 0:
            settle(early_in, e_recv.at[0])
            early_sum[0] = early_out[0] + early_in[0]
            early_sum[1] = early_out[1] + early_in[1]
            early_sum[2] = slot_ids + bad
            remote(early_sum, early_low, e_send.at[1], e_recv.at[1], nearby[HALF]).start()
            remote(
                early_sum.at[pl.ds(0, 2)], early_high, e_send.at[2], e_recv.at[2], nearby[-HALF]
            ).start()
    part_out[...] = jnp.transpose(dots)[0:NZ]

    for c in (core, 1 - core):
        remote(part_out, part_in.at[core], part_send, part_recv, ring(HALF, c)).start()
        remote(part_out, part_in.at[2 + core], part_send, part_recv, ring(-HALF, c)).start()
    settle(early_low, e_recv.at[1])
    settle(early_high, e_recv.at[2])
    inverse_t = lax.rsqrt(early_low[0] + early_high[0] + epsilon)
    inverse_c = lax.rsqrt(early_low[1] + early_high[1] + epsilon)
    mid_ids = early_low[2]
    bad = jnp.max(jnp.max(mid_ids, axis=1, keepdims=True), axis=0, keepdims=True) >= MARK * 0.5
    bad = jnp.where(bad, MARK, 0.0)
    turned = down(mid_ids)
    for k in range(NZ):
        mid_wide[k] = jnp.broadcast_to(turned[:, k : k + 1], (ROW, ROW))
    settle(part_in, part_recv)
    dot = (part_in[0] + part_in[1]) + (part_in[2] + part_in[3])
    match = jax.nn.sigmoid(logit_scale * dot * inverse_t * inverse_c)
    match = jnp.where(mid_ids >= 0.0, match, 0.0)

    match_turned = down(match)
    counts = [jnp.zeros((SLOT, ROW), f32) for _ in range(NZ)]
    for m in range(NZ):
        weight = jnp.broadcast_to(match_turned[:, m : m + 1], (ROW, ROW))
        theirs = mid_wide[m]
        for k in range(NZ):
            same = jnp.where(theirs == mid_ids[k : k + 1], weight, 0.0)
            counts[k] = counts[k] + jnp.sum(same.reshape(ROW // SLOT, SLOT, ROW), axis=0)
    count = jnp.concatenate([jnp.sum(c, axis=0, keepdims=True) for c in counts], axis=0)
    capped = CAP * 1.0
    balanced = match * capped / jnp.maximum(count, capped) + bad

    for k in range(NZ):
        back_out[(k + HALF) % NZ] = balanced[k : k + 1]
    for k in (0, 7, 1, 6, 2, 5, 3):
        i = (k + HALF) % NZ
        remote(back_out.at[i], back_mid.at[i], bz_send, bz_recv, nearby[HALF - k]).start()
    settle(back_mid.at[pl.ds(1, NZ - 1)], bz_recv)
    back_tile[...] = jnp.concatenate(
        [back_out[0] if k == HALF else back_mid[(k + HALF) % NZ] for k in range(NZ)], axis=0
    )
    for j in range(1, PLANE):
        remote(back_tile, back_in.at[j], bt_send, bt_recv, peer_back[j]).start()
    at_slot = one_hot(slots == lane)
    settle(back_in.at[pl.ds(1, PLANE - 1)], bt_recv)
    group = lax.broadcasted_iota(i32, (NZ, ROW), 1) // SLOT
    given = back_tile[...]
    highest = given
    for j in range(1, PLANE):
        theirs = back_in[j]
        given = jnp.where(group == j, theirs, given)
        highest = jnp.maximum(highest, theirs)
    flag_ref[0] = jnp.where(jnp.max(highest) >= MARK * 0.5, 1, 0)
    looked = jnp.dot(
        jnp.concatenate(thirds(given), axis=0).astype(bf16), at_slot, preferred_element_type=f32
    )
    looked = (looked[0:NZ] + looked[NZ : 2 * NZ]) + looked[2 * NZ : 3 * NZ]
    at_block = lax.broadcasted_iota(i32, (NZ, pairs), 0)
    out_ref[...] = jnp.sum(jnp.where(at_block == to_z, looked, 0.0), axis=0, keepdims=True)

    settle(meta_out.at[pl.ds(1, NZ - 1)], mz_send)
    settle(sent, z_send)
    if packed:
        settle(late_sent, late_send)
        settle(taken_in.at[pl.ds(1, PLANE - 1)], taken_send)
    settle(landed.at[:, pl.ds(1, PLANE - 1)], xy_send)
    settle(meta_in.at[pl.ds(1, PLANE - 1)], mt_send)
    settle(early_out, e_send.at[0])
    settle(early_low, e_send.at[1])
    settle(early_high, e_send.at[2])
    settle(part_in, part_send)
    settle(back_out.at[pl.ds(1, NZ - 1)], bz_send)
    settle(back_in.at[pl.ds(1, PLANE - 1)], bt_send)


def curate(packed, text, concept_table, ids):
    pairs, quarter = text.shape
    held = concept_table.shape[0]
    vmem, dma = pltpu.VMEM, pltpu.SemaphoreType.DMA
    blocks = (NZ, PLANE, SLOT, quarter)
    piece = (PLANE, SLOT, quarter)
    fast, slow = len(Z_FIRST), len(PLANE_FIRST)
    moved = (fast, packed, quarter) if packed else (NZ - 1, *piece)
    return pl.pallas_call(
        functools.partial(kernel, packed),
        name="curate_packed" if packed else "curate_whole",
        out_shape=(
            jax.ShapeDtypeStruct((1, pairs), f32),
            jax.ShapeDtypeStruct((1,), i32),
        ),
        in_specs=[
            pl.BlockSpec(memory_space=pl.ANY),
            pl.BlockSpec(memory_space=pl.ANY),
            pl.BlockSpec(memory_space=pl.ANY),
        ],
        out_specs=(
            pl.BlockSpec(memory_space=pltpu.VMEM),
            pl.BlockSpec(memory_space=pltpu.SMEM),
        ),
        scratch_shapes=[
            vmem((1, pairs), i32),
            vmem((pairs, quarter), bf16),
            vmem((held, quarter), bf16),
            vmem((1 + slow if packed else 1, *piece), bf16),
            vmem(moved, bf16),
            vmem(moved, bf16),
            vmem((fast, *piece) if packed else (1, 1, SLOT, quarter), bf16),
            vmem((fast, ROW, packed) if packed else (1, SLOT, ROW), bf16),
            vmem(blocks, bf16),
            vmem((slow, PACKED_LATE, quarter), bf16),
            vmem((slow, PACKED_LATE, quarter), bf16),
            vmem((slow, ROW, PACKED_LATE), bf16),
            vmem((PLANE, SLOT, ROW), bf16),
            vmem((PLANE, SLOT, ROW), bf16),
            vmem((NZ, 2, ROW), f32),
            vmem((NZ, 2, ROW), f32),
            vmem((PLANE, SLOT, ROW), f32),
            vmem((PLANE, SLOT, ROW), f32),
            vmem((NZ, ROW, ROW), f32),
            vmem((ROW, held), bf16),
            vmem((NZ, ROW, quarter), f32),
            vmem((2, NZ, ROW), f32),
            vmem((2, NZ, ROW), f32),
            vmem((3, NZ, ROW), f32),
            vmem((3, NZ, ROW), f32),
            vmem((2, NZ, ROW), f32),
            vmem((NZ, ROW, ROW), f32),
            vmem((NZ, ROW), f32),
            vmem((4, NZ, ROW), f32),
            vmem((NZ, 1, ROW), f32),
            vmem((NZ, 1, ROW), f32),
            vmem((NZ, ROW), f32),
            vmem((PLANE, NZ, ROW), f32),
            dma((3,)),
            dma, dma((NZ,)), dma, dma, dma, dma, dma, dma((NZ,)),
            dma((3,)), dma((3,)), dma, dma, dma, dma, dma, dma,
            dma, dma, dma,
        ],
        compiler_params=pltpu.CompilerParams(
            collective_id=1 if packed else 0, has_side_effects=True
        ),
    )(text, concept_table, ids)


def body(text, concept_table, ids):
    pairs = text.shape[0]
    line = ids.reshape(1, pairs)
    out, over = curate(PACKED, text, concept_table, line)
    out = lax.cond(
        over[0] > 0,
        lambda: curate(0, text, concept_table, line)[0],
        lambda: out,
    )
    return out.reshape(pairs)


def solution(mesh):
    placed = (P("dp", "concept"), P("dp", "concept"), P("dp"))
    return jax.shard_map(body, mesh=mesh, in_specs=placed, out_specs=P("dp"), check_vma=False)
```

```python
import functools

import jax
import jax.numpy as jnp
from jax import lax
from jax.experimental import pallas as pl
from jax.experimental.pallas import tpu as pltpu
from jax.sharding import PartitionSpec as P

CAP = 16
SLOT = 8
NX, NZ, NY = 4, 8, 4
PLANE = NX * NY
ROW = PLANE * SLOT
Z_ORDER = (4, 3, 5, 2, 6, 1, 7)
Z_FIRST = (4, 3, 5)
PLANE_FIRST = (2, 6, 1, 7)
PACKED = 88
PACKED_LATE = 96
MARK = 8192.0
HALF = NZ // 2

logit_scale = 64.0
epsilon = 1e-06
f32, bf16, i32 = jnp.float32, jnp.bfloat16, jnp.int32


def one_hot(test):
    return jnp.where(test, 1.0, 0.0).astype(bf16)


def thirds(x):
    high = x.astype(bf16).astype(f32)
    middle = (x - high).astype(bf16).astype(f32)
    low = x - high - middle
    return [high, middle, low]


def down(square):
    filler = jnp.zeros((ROW - square.shape[0], ROW), f32)
    return jnp.transpose(jnp.concatenate([square, filler], axis=0))


def kernel(
    packed, text_hbm, table_hbm, ids_hbm, out_ref, flag_ref,
    ids_ref, text_v, table_v, kept, sent, carried, spread, spreaders, landed,
    late_sent, late_carried, late_spreaders, taken_out, taken_in,
    meta_out, meta_mid, meta_tile, meta_in, ids_wide, hot, pieces,
    early_out, early_in, early_sum, early_low, early_high, early_half, early_other, mid_wide,
    mark_out, mark_plane, mark_sum, mark_z,
    part_out, part_in, back_out, back_mid, back_tile, back_in,
    load_sem, z_send, z_recv, mz_send, mz_recv, mt_send, mt_recv, xy_send, xy_recv,
    e_send, e_recv, part_send, part_recv, bz_send, bz_recv, bt_send, bt_recv,
    late_send, taken_send, taken_recv, mp_send, mp_recv, mk_send, mk_recv,
):
    pairs = ids_ref.shape[1]
    held = table_v.shape[0]
    first = Z_FIRST if packed else Z_ORDER
    late = PLANE_FIRST if packed else ()
    me = lax.axis_index("dp")
    mine = lax.axis_index("concept")
    my_x, my_z, my_y = lax.div(me, NZ * NY), lax.rem(lax.div(me, NY), NZ), lax.rem(me, NY)
    core = lax.rem(mine, 2)
    partner = mine + 1 - 2 * core
    my_ring = lax.div(mine, 2) * NZ + my_z

    z_peer = [(me + (lax.rem(my_z + k, NZ) - my_z) * NY, mine) for k in range(NZ)]
    x_step = [(lax.rem(my_x + d, NX) - my_x) * (NZ * NY) for d in range(NX)]
    y_step = [lax.rem(my_y + d, NY) - my_y for d in range(NY)]
    peer = [(me + x_step[j // NY] + y_step[j % NY], mine) for j in range(PLANE)]
    peer_back = [peer[(-(j // NY)) % NX * NY + (-j) % NY] for j in range(PLANE)]
    other_core = (me, partner)

    def ring(step, on_core):
        there = lax.rem(my_ring + step + 2 * NZ, 2 * NZ)
        return (me + (lax.rem(there, NZ) - my_z) * NY, lax.div(there, NZ) * 2 + on_core)

    nearby = {e: ring(e, core) for e in range(-HALF, HALF + 1)}

    def remote(src, dst, send, recv, device):
        return pltpu.make_async_remote_copy(
            src_ref=src, dst_ref=dst, send_sem=send, recv_sem=recv,
            device_id=device, device_id_type=pl.DeviceIdType.MESH,
        )

    def settle(ref, sem):
        pltpu.make_async_copy(ref, ref, sem).wait()

    barrier = pltpu.get_barrier_semaphore()

    def greet(device):
        pl.semaphore_signal(
            barrier, inc=1, device_id=device, device_id_type=pl.DeviceIdType.MESH
        )

    load_text = pltpu.make_async_copy(text_hbm, text_v, load_sem.at[0])
    load_ids = pltpu.make_async_copy(ids_hbm, ids_ref, load_sem.at[2])
    load_ids.start()
    for k in Z_ORDER:
        greet(z_peer[k])
    for j in range(1, PLANE):
        greet(peer[j])
    for e in range(1, HALF + 1):
        greet(nearby[e])
        greet(nearby[-e])
    greet(ring(HALF, 1 - core))
    greet(ring(-HALF, 1 - core))
    greet(other_core)
    load_text.start()
    load_table = pltpu.make_async_copy(table_hbm, table_v, load_sem.at[1])
    load_table.start()

    load_ids.wait()
    ids = ids_ref[...]
    owner = ((ids >> 10) * 43691) >> 17
    local = ids - owner * held
    to_z = (((owner >> 2) & 7) - my_z) & 7
    to_plane = ((((owner >> 5) - my_x) & 3) << 2) | (((owner & 3) - my_y) & 3)
    relative = to_z * PLANE + to_plane
    owners = lax.broadcasted_iota(i32, (NZ * PLANE, pairs), 0)
    is_owner = jnp.where(owners == relative, 1.0, 0.0)
    earlier = one_hot(
        lax.broadcasted_iota(i32, (pairs, pairs), 0)
        < lax.broadcasted_iota(i32, (pairs, pairs), 1)
    )
    is_owner_low = is_owner.astype(bf16)
    ahead = jnp.dot(is_owner_low, earlier, preferred_element_type=f32)
    rank = jnp.sum(is_owner * ahead, axis=0, keepdims=True).astype(i32)
    lane = to_plane * SLOT + rank
    target = to_z * ROW + lane
    mark = 0.0
    if packed:
        down_i = lax.broadcasted_iota(i32, (NZ * PLANE, NZ * PLANE), 0)
        over_i = lax.broadcasted_iota(i32, (NZ * PLANE, NZ * PLANE), 1)
        before = one_hot((over_i < down_i) & ((over_i >> 4) == (down_i >> 4)))
        held_by = jnp.sum(is_owner, axis=1, keepdims=True)
        held_by = jnp.broadcast_to(held_by, (NZ * PLANE, ROW)).astype(bf16)
        base = jnp.dot(before, held_by, preferred_element_type=f32)[:, 0:1]
        place = rank + jnp.sum(is_owner * base, axis=0, keepdims=True).astype(i32)
        full = jnp.max(place.astype(f32), axis=1, keepdims=True)
        mark = jnp.where(full >= float(packed), MARK, 0.0)
        place = to_z * ROW + place

    load_text.wait()
    ones = jnp.ones((SLOT, text_v.shape[1]), bf16)
    words = text_v[...].astype(f32)
    squares = words * words
    squares_high = squares.astype(bf16)
    squares_low = (squares - squares_high.astype(f32)).astype(bf16)
    across_lanes = (((1,), (1,)), ((), ()))
    tsq_pair = lax.dot_general(
        ones, squares_high, across_lanes, preferred_element_type=f32
    ) + lax.dot_general(ones, squares_low, across_lanes, preferred_element_type=f32)
    values = jnp.concatenate(
        [
            (local >> 6).astype(f32),
            (local & 63).astype(f32),
            jnp.ones((1, pairs), f32),
            *thirds(tsq_pair[0:1]),
            jnp.zeros((2, pairs), f32),
        ],
        axis=0,
    ).astype(bf16)
    slots = lax.broadcasted_iota(i32, (ROW, pairs), 0)
    taken_rows = {}
    for k in range(NZ):
        pick = one_hot(slots + k * ROW == target)
        meta = lax.dot_general(values, pick, across_lanes, preferred_element_type=f32)
        meta_out[k] = jnp.concatenate(
            [
                meta[0:1] * 64.0 + meta[1:2] + meta[2:3] - 1.0 + mark,
                (meta[3:4] + meta[4:5]) + meta[5:6],
            ],
            axis=0,
        )
        taken_rows[k] = meta[2:3]
        if k == 0 or k in late:
            at = (late.index(k) + 1) if k else 0
            block = jnp.dot(pick, text_v[...], preferred_element_type=f32)
            kept[at] = block.reshape(PLANE, SLOT, -1).astype(bf16)
    if packed:
        filler = jnp.zeros((SLOT - len(late), ROW), f32)
        tile = jnp.concatenate([taken_rows[k] for k in late] + [filler], axis=0)
        taken_out[...] = down(tile).reshape(PLANE, SLOT, ROW).astype(bf16)

    pl.semaphore_wait(barrier, NZ - 1 + PLANE - 1 + 2 * HALF + 3)

    for k in Z_ORDER:
        remote(meta_out.at[k], meta_mid.at[k], mz_send, mz_recv, z_peer[k]).start()
    for i, k in enumerate(first):
        if packed:
            pick = one_hot(slots[0:packed] + k * ROW == place)
        else:
            pick = one_hot(slots + k * ROW == target)
        block = jnp.dot(pick, text_v[...], preferred_element_type=f32)
        sent[i] = block.astype(bf16).reshape(sent.shape[1:])
        remote(sent.at[i], carried.at[i], z_send, z_recv.at[k], z_peer[k]).start()

    def pass_on(source, k):
        for j in range(1, PLANE):
            remote(source.at[j], landed.at[k, j], xy_send, xy_recv.at[k], peer[j]).start()

    if packed:
        for j in range(1, PLANE):
            remote(taken_out.at[j], taken_in.at[j], taken_send, taken_recv, peer[j]).start()
    for i, k in enumerate(late):
        pass_on(kept.at[i + 1], k)
    pass_on(kept.at[0], 0)

    def arrived(k, own):
        settle(landed.at[k, pl.ds(1, PLANE - 1)], xy_recv.at[k])
        return jnp.concatenate(
            [own[0:1].astype(f32), landed[k, 1:PLANE].astype(f32)], axis=0
        ).reshape(ROW, -1)

    over = one_hot(
        lax.broadcasted_iota(i32, (ROW, ROW), 0) < lax.broadcasted_iota(i32, (ROW, ROW), 1)
    )

    def places(taken):
        spot = jnp.dot(one_hot(taken), over, preferred_element_type=f32)
        return jnp.where(taken, spot, -1.0)

    settle(meta_mid.at[pl.ds(1, NZ - 1)], mz_recv)
    metas = [meta_out[0]] + [meta_mid[k] for k in range(1, NZ)]
    tile = jnp.concatenate([m[0:1] for m in metas] + [m[1:2] for m in metas], axis=0)
    if packed:
        tile = jnp.concatenate([tile, places(tile[0:NZ] >= 0.0)], axis=0)
    turned = down(tile)
    meta_tile[...] = turned.reshape(PLANE, SLOT, ROW)
    for j in range(1, PLANE):
        remote(meta_tile.at[j], meta_in.at[j], mt_send, mt_recv, peer[j]).start()
    if packed:
        lanes = lax.broadcasted_iota(i32, (ROW, packed), 1).astype(f32)
        for i, k in enumerate(first):
            at = 2 * NZ + k
            spreaders[i] = one_hot(turned[:, at : at + 1] == lanes)

    def expand_and_pass(i):
        k = first[i]
        settle(carried.at[i], z_recv.at[k])
        if packed:
            block = jnp.dot(spreaders[i], carried[i], preferred_element_type=f32)
            spread[i] = block.reshape(PLANE, SLOT, -1).astype(bf16)
            pass_on(spread.at[i], k)
        else:
            pass_on(carried.at[i], k)

    if packed:
        settle(taken_in.at[pl.ds(1, PLANE - 1)], taken_recv)
        theirs = jnp.concatenate(
            [taken_out[0:1].astype(f32), taken_in[1:PLANE].astype(f32)], axis=0
        ).reshape(ROW, ROW)
        late_place = places(jnp.transpose(theirs)[0:NZ] > 0.5)
        late_rows = lax.broadcasted_iota(i32, (PACKED_LATE, ROW), 0).astype(f32)

    def pack_late(i):
        k = late[i]
        block = arrived(k, kept.at[i + 1]).astype(bf16)
        pick = one_hot(late_rows == late_place[i : i + 1])
        late_sent[i] = jnp.dot(pick, block, preferred_element_type=f32).astype(bf16)
        remote(late_sent.at[i], late_carried.at[i], late_send, z_recv.at[k], z_peer[k]).start()

    for i in range(len(late)):
        pack_late(i)
    expand_and_pass(0)

    settle(meta_in.at[pl.ds(1, PLANE - 1)], mt_recv)
    theirs = jnp.concatenate([meta_tile[0:1], meta_in[1:PLANE]], axis=0).reshape(ROW, ROW)
    by_row = jnp.transpose(theirs)
    slot_ids, tsq_part = by_row[0:NZ], by_row[NZ : 2 * NZ]
    bad = jnp.max(jnp.max(slot_ids, axis=1, keepdims=True), axis=0, keepdims=True) >= MARK * 0.5
    if packed:
        here = places(slot_ids >= 0.0)
        late_here = jnp.concatenate([here[k : k + 1] for k in late], axis=0)
        most = jnp.max(jnp.max(late_here, axis=1, keepdims=True), axis=0, keepdims=True)
        bad = bad | (most >= float(PACKED_LATE))
        turned = down(here)
        lanes = lax.broadcasted_iota(i32, (ROW, PACKED_LATE), 1).astype(f32)
        for i, k in enumerate(late):
            late_spreaders[i] = one_hot(turned[:, k : k + 1] == lanes)
    mark_out[...] = jnp.broadcast_to(jnp.where(bad, 1.0, 0.0), (1, ROW))
    for j in range(1, PLANE):
        remote(mark_out, mark_plane.at[j], mp_send, mp_recv, peer[j]).start()
    for k in range(NZ):
        ids_wide[k] = jnp.broadcast_to(theirs[:, k : k + 1], (ROW, ROW))

    load_table.wait()
    columns = lax.broadcasted_iota(i32, (ROW, ROW), 1)
    columns_f = columns.astype(f32)

    def fetch(k, csq_cols):
        wanted = ids_wide[k]
        for c in range(held // ROW):
            hot[:, c * ROW : (c + 1) * ROW] = one_hot(wanted - float(c * ROW) == columns_f)
        piece = jnp.dot(hot[...], table_v[...], preferred_element_type=f32)
        pieces[k] = piece
        return jnp.where(columns == k, jnp.sum(piece * piece, axis=1, keepdims=True), csq_cols)

    csq_cols = jnp.zeros((ROW, ROW), f32)
    for step in range(4):
        csq_cols = lax.fori_loop(2 * step, 2 * step + 2, fetch, csq_cols)
        if 1 + step < len(first):
            expand_and_pass(1 + step)
    settle(mark_plane.at[pl.ds(1, PLANE - 1)], mp_recv)
    worst = mark_out[...]
    for j in range(1, PLANE):
        worst = jnp.maximum(worst, mark_plane[j])
    mark_sum[...] = worst
    early_out[0] = tsq_part
    early_out[1] = jnp.transpose(csq_cols)[0:NZ]

    remote(early_out.at[1 - core], early_in, e_send.at[0], e_recv.at[0], other_core).start()
    for i in range(5, len(first)):
        expand_and_pass(i)

    for k in Z_ORDER:
        remote(mark_sum, mark_z.at[k], mk_send, mk_recv, z_peer[k]).start()

    dots = jnp.zeros((ROW, ROW), f32)
    for k in (0,) + first + late:
        if k in late:
            i = late.index(k)
            settle(late_carried.at[i], z_recv.at[k])
            words = jnp.dot(late_spreaders[i], late_carried[i], preferred_element_type=f32)
        elif k == 0:
            words = arrived(k, kept.at[0])
        else:
            i = first.index(k)
            words = arrived(k, spread.at[i] if packed else carried.at[i])
        total = jnp.sum(words * pieces[k], axis=1, keepdims=True)
        dots = jnp.where(columns == k, total, dots)
        if k == 0:
            settle(early_in, e_recv.at[0])
            early_sum[0] = early_out[core] + early_in[...]
            early_sum[1] = slot_ids
            remote(early_sum, early_low, e_send.at[1], e_recv.at[1], nearby[HALF]).start()
            remote(
                early_sum.at[0], early_high, e_send.at[2], e_recv.at[2], nearby[-HALF]
            ).start()
    part_out[...] = jnp.transpose(dots)[0:NZ]

    for c in (core, 1 - core):
        remote(part_out, part_in.at[core], part_send, part_recv, ring(HALF, c)).start()
        remote(part_out, part_in.at[2 + core], part_send, part_recv, ring(-HALF, c)).start()
    settle(early_low, e_recv.at[1])
    settle(early_high, e_recv.at[2])
    early_half[...] = early_low[0] + early_high[...]
    mid_ids = early_low[1]
    turned = down(mid_ids)
    for k in range(NZ):
        mid_wide[k] = jnp.broadcast_to(turned[:, k : k + 1], (ROW, ROW))
    remote(early_half, early_other, e_send.at[3], e_recv.at[3], other_core).start()
    settle(mark_z.at[pl.ds(1, NZ - 1)], mk_recv)
    worst = mark_sum[...]
    for k in range(1, NZ):
        worst = jnp.maximum(worst, mark_z[k])
    flag_ref[0] = jnp.where(jnp.max(worst) > 0.5, 1, 0)
    settle(early_other, e_recv.at[3])
    half, other = early_half[...], early_other[...]
    inverse_t = lax.rsqrt(jnp.where(core == 0, half, other) + epsilon)
    inverse_c = lax.rsqrt(jnp.where(core == 0, other, half) + epsilon)
    settle(part_in, part_recv)
    dot = (part_in[0] + part_in[1]) + (part_in[2] + part_in[3])
    match = jax.nn.sigmoid(logit_scale * dot * inverse_t * inverse_c)
    match = jnp.where(mid_ids >= 0.0, match, 0.0)

    match_turned = down(match)
    counts = [jnp.zeros((SLOT, ROW), f32) for _ in range(NZ)]
    for m in range(NZ):
        weight = jnp.broadcast_to(match_turned[:, m : m + 1], (ROW, ROW))
        theirs = mid_wide[m]
        for k in range(NZ):
            same = jnp.where(theirs == mid_ids[k : k + 1], weight, 0.0)
            counts[k] = counts[k] + jnp.sum(same.reshape(ROW // SLOT, SLOT, ROW), axis=0)
    count = jnp.concatenate([jnp.sum(c, axis=0, keepdims=True) for c in counts], axis=0)
    capped = CAP * 1.0
    balanced = match * capped / jnp.maximum(count, capped)

    for k in range(NZ):
        back_out[(k + HALF) % NZ] = balanced[k : k + 1]
    for k in (0, 7, 1, 6, 2, 5, 3):
        i = (k + HALF) % NZ
        remote(back_out.at[i], back_mid.at[i], bz_send, bz_recv, nearby[HALF - k]).start()
    settle(back_mid.at[pl.ds(1, NZ - 1)], bz_recv)
    back_tile[...] = jnp.concatenate(
        [back_out[0] if k == HALF else back_mid[(k + HALF) % NZ] for k in range(NZ)], axis=0
    )
    for j in range(1, PLANE):
        remote(back_tile, back_in.at[j], bt_send, bt_recv, peer_back[j]).start()
    at_slot = one_hot(slots == lane)
    settle(back_in.at[pl.ds(1, PLANE - 1)], bt_recv)
    group = lax.broadcasted_iota(i32, (NZ, ROW), 1) // SLOT
    given = back_tile[...]
    for j in range(1, PLANE):
        given = jnp.where(group == j, back_in[j], given)
    looked = jnp.dot(
        jnp.concatenate(thirds(given), axis=0).astype(bf16), at_slot, preferred_element_type=f32
    )
    looked = (looked[0:NZ] + looked[NZ : 2 * NZ]) + looked[2 * NZ : 3 * NZ]
    at_block = lax.broadcasted_iota(i32, (NZ, pairs), 0)
    out_ref[...] = jnp.sum(jnp.where(at_block == to_z, looked, 0.0), axis=0, keepdims=True)

    settle(meta_out.at[pl.ds(1, NZ - 1)], mz_send)
    settle(sent, z_send)
    if packed:
        settle(late_sent, late_send)
        settle(taken_in.at[pl.ds(1, PLANE - 1)], taken_send)
    settle(landed.at[:, pl.ds(1, PLANE - 1)], xy_send)
    settle(meta_in.at[pl.ds(1, PLANE - 1)], mt_send)
    settle(early_in, e_send.at[0])
    settle(early_other, e_send.at[3])
    settle(mark_plane.at[pl.ds(1, PLANE - 1)], mp_send)
    settle(mark_z.at[pl.ds(1, NZ - 1)], mk_send)
    settle(early_low, e_send.at[1])
    settle(early_high, e_send.at[2])
    settle(part_in, part_send)
    settle(back_out.at[pl.ds(1, NZ - 1)], bz_send)
    settle(back_in.at[pl.ds(1, PLANE - 1)], bt_send)


def curate(packed, text, concept_table, ids):
    pairs, quarter = text.shape
    held = concept_table.shape[0]
    vmem, dma = pltpu.VMEM, pltpu.SemaphoreType.DMA
    blocks = (NZ, PLANE, SLOT, quarter)
    piece = (PLANE, SLOT, quarter)
    fast, slow = len(Z_FIRST), len(PLANE_FIRST)
    moved = (fast, packed, quarter) if packed else (NZ - 1, *piece)
    return pl.pallas_call(
        functools.partial(kernel, packed),
        name="curate_packed" if packed else "curate_whole",
        out_shape=(
            jax.ShapeDtypeStruct((1, pairs), f32),
            pltpu.SMEM((1,), i32),
        ),
        in_specs=[
            pl.BlockSpec(memory_space=pl.ANY),
            pl.BlockSpec(memory_space=pl.ANY),
            pl.BlockSpec(memory_space=pl.ANY),
        ],
        out_specs=(
            pl.BlockSpec(memory_space=pltpu.VMEM),
            pl.BlockSpec(memory_space=pltpu.SMEM),
        ),
        scratch_shapes=[
            vmem((1, pairs), i32),
            vmem((pairs, quarter), bf16),
            vmem((held, quarter), bf16),
            vmem((1 + slow if packed else 1, *piece), bf16),
            vmem(moved, bf16),
            vmem(moved, bf16),
            vmem((fast, *piece) if packed else (1, 1, SLOT, quarter), bf16),
            vmem((fast, ROW, packed) if packed else (1, SLOT, ROW), bf16),
            vmem(blocks, bf16),
            vmem((slow, PACKED_LATE, quarter), bf16),
            vmem((slow, PACKED_LATE, quarter), bf16),
            vmem((slow, ROW, PACKED_LATE), bf16),
            vmem((PLANE, SLOT, ROW), bf16),
            vmem((PLANE, SLOT, ROW), bf16),
            vmem((NZ, 2, ROW), f32),
            vmem((NZ, 2, ROW), f32),
            vmem((PLANE, SLOT, ROW), f32),
            vmem((PLANE, SLOT, ROW), f32),
            vmem((NZ, ROW, ROW), f32),
            vmem((ROW, held), bf16),
            vmem((NZ, ROW, quarter), f32),
            vmem((2, NZ, ROW), f32),
            vmem((NZ, ROW), f32),
            vmem((2, NZ, ROW), f32),
            vmem((2, NZ, ROW), f32),
            vmem((NZ, ROW), f32),
            vmem((NZ, ROW), f32),
            vmem((NZ, ROW), f32),
            vmem((NZ, ROW, ROW), f32),
            vmem((1, ROW), f32),
            vmem((PLANE, 1, ROW), f32),
            vmem((1, ROW), f32),
            vmem((NZ, 1, ROW), f32),
            vmem((NZ, ROW), f32),
            vmem((4, NZ, ROW), f32),
            vmem((NZ, 1, ROW), f32),
            vmem((NZ, 1, ROW), f32),
            vmem((NZ, ROW), f32),
            vmem((PLANE, NZ, ROW), f32),
            dma((3,)),
            dma, dma((NZ,)), dma, dma, dma, dma, dma, dma((NZ,)),
            dma((4,)), dma((4,)), dma, dma, dma, dma, dma, dma,
            dma, dma, dma, dma, dma, dma, dma,
        ],
        compiler_params=pltpu.CompilerParams(
            collective_id=1 if packed else 0, has_side_effects=True
        ),
    )(text, concept_table, ids)


def body(text, concept_table, ids):
    pairs = text.shape[0]
    line = ids.reshape(1, pairs)
    out, over = curate(PACKED, text, concept_table, line)
    out = lax.cond(
        over[0] > 0,
        lambda: curate(0, text, concept_table, line)[0],
        lambda: out,
    )
    return out.reshape(pairs)


def solution(mesh):
    placed = (P("dp", "concept"), P("dp", "concept"), P("dp"))
    return jax.shard_map(body, mesh=mesh, in_specs=placed, out_specs=P("dp"), check_vma=False)
```

```python
import functools

import jax
import jax.numpy as jnp
from jax import lax
from jax.experimental import pallas as pl
from jax.experimental.pallas import tpu as pltpu
from jax.sharding import PartitionSpec as P

CAP = 16
SLOT = 8
NX, NZ, NY = 4, 8, 4
PLANE = NX * NY
ROW = PLANE * SLOT
Z_ORDER = (4, 3, 5, 2, 6, 1, 7)
Z_FIRST = (4,)
PLANE_FIRST = (3, 5, 2, 6, 1, 7)
PACKED = 88
PACKED_LATE = 96
MARK = 8192.0
HALF = NZ // 2

logit_scale = 64.0
epsilon = 1e-06
f32, bf16, i32 = jnp.float32, jnp.bfloat16, jnp.int32


def one_hot(test):
    return jnp.where(test, 1.0, 0.0).astype(bf16)


def thirds(x):
    high = x.astype(bf16).astype(f32)
    middle = (x - high).astype(bf16).astype(f32)
    low = x - high - middle
    return [high, middle, low]


def down(square):
    filler = jnp.zeros((ROW - square.shape[0], ROW), f32)
    return jnp.transpose(jnp.concatenate([square, filler], axis=0))


def kernel(
    packed, text_hbm, table_hbm, ids_hbm, out_ref, flag_ref,
    ids_ref, text_v, table_v, kept, sent, carried, spread, spreaders, landed,
    late_sent, late_carried, late_spreaders, taken_out, taken_in,
    meta_out, meta_mid, meta_tile, meta_in, ids_wide, hot, pieces,
    early_out, early_in, early_sum, early_low, early_high, early_half, early_other, mid_wide,
    mark_out, mark_plane, mark_sum, mark_z,
    part_out, part_in, back_out, back_mid, back_tile, back_in,
    load_sem, z_send, z_recv, mz_send, mz_recv, mt_send, mt_recv, xy_send, xy_recv,
    e_send, e_recv, part_send, part_recv, bz_send, bz_recv, bt_send, bt_recv,
    late_send, taken_send, taken_recv, mp_send, mp_recv, mk_send, mk_recv,
):
    pairs = ids_ref.shape[1]
    held = table_v.shape[0]
    first = Z_FIRST if packed else Z_ORDER
    late = PLANE_FIRST if packed else ()
    me = lax.axis_index("dp")
    mine = lax.axis_index("concept")
    my_x, my_z, my_y = lax.div(me, NZ * NY), lax.rem(lax.div(me, NY), NZ), lax.rem(me, NY)
    core = lax.rem(mine, 2)
    partner = mine + 1 - 2 * core
    my_ring = lax.div(mine, 2) * NZ + my_z

    z_peer = [(me + (lax.rem(my_z + k, NZ) - my_z) * NY, mine) for k in range(NZ)]
    x_step = [(lax.rem(my_x + d, NX) - my_x) * (NZ * NY) for d in range(NX)]
    y_step = [lax.rem(my_y + d, NY) - my_y for d in range(NY)]
    peer = [(me + x_step[j // NY] + y_step[j % NY], mine) for j in range(PLANE)]
    peer_back = [peer[(-(j // NY)) % NX * NY + (-j) % NY] for j in range(PLANE)]
    other_core = (me, partner)

    def ring(step, on_core):
        there = lax.rem(my_ring + step + 2 * NZ, 2 * NZ)
        return (me + (lax.rem(there, NZ) - my_z) * NY, lax.div(there, NZ) * 2 + on_core)

    nearby = {e: ring(e, core) for e in range(-HALF, HALF + 1)}

    def remote(src, dst, send, recv, device):
        return pltpu.make_async_remote_copy(
            src_ref=src, dst_ref=dst, send_sem=send, recv_sem=recv,
            device_id=device, device_id_type=pl.DeviceIdType.MESH,
        )

    def settle(ref, sem):
        pltpu.make_async_copy(ref, ref, sem).wait()

    barrier = pltpu.get_barrier_semaphore()

    def greet(device):
        pl.semaphore_signal(
            barrier, inc=1, device_id=device, device_id_type=pl.DeviceIdType.MESH
        )

    load_text = pltpu.make_async_copy(text_hbm, text_v, load_sem.at[0])
    load_ids = pltpu.make_async_copy(ids_hbm, ids_ref, load_sem.at[2])
    load_ids.start()
    for k in Z_ORDER:
        greet(z_peer[k])
    for j in range(1, PLANE):
        greet(peer[j])
    for e in range(1, HALF + 1):
        greet(nearby[e])
        greet(nearby[-e])
    greet(ring(HALF, 1 - core))
    greet(ring(-HALF, 1 - core))
    greet(other_core)
    load_text.start()
    load_table = pltpu.make_async_copy(table_hbm, table_v, load_sem.at[1])
    load_table.start()

    load_ids.wait()
    ids = ids_ref[...]
    owner = ((ids >> 10) * 43691) >> 17
    local = ids - owner * held
    to_z = (((owner >> 2) & 7) - my_z) & 7
    to_plane = ((((owner >> 5) - my_x) & 3) << 2) | (((owner & 3) - my_y) & 3)
    relative = to_z * PLANE + to_plane
    owners = lax.broadcasted_iota(i32, (NZ * PLANE, pairs), 0)
    is_owner = jnp.where(owners == relative, 1.0, 0.0)
    earlier = one_hot(
        lax.broadcasted_iota(i32, (pairs, pairs), 0)
        < lax.broadcasted_iota(i32, (pairs, pairs), 1)
    )
    is_owner_low = is_owner.astype(bf16)
    ahead = jnp.dot(is_owner_low, earlier, preferred_element_type=f32)
    rank = jnp.sum(is_owner * ahead, axis=0, keepdims=True).astype(i32)
    lane = to_plane * SLOT + rank
    target = to_z * ROW + lane
    mark = 0.0
    if packed:
        down_i = lax.broadcasted_iota(i32, (NZ * PLANE, NZ * PLANE), 0)
        over_i = lax.broadcasted_iota(i32, (NZ * PLANE, NZ * PLANE), 1)
        before = one_hot((over_i < down_i) & ((over_i >> 4) == (down_i >> 4)))
        held_by = jnp.sum(is_owner, axis=1, keepdims=True)
        held_by = jnp.broadcast_to(held_by, (NZ * PLANE, ROW)).astype(bf16)
        base = jnp.dot(before, held_by, preferred_element_type=f32)[:, 0:1]
        place = rank + jnp.sum(is_owner * base, axis=0, keepdims=True).astype(i32)
        full = jnp.max(place.astype(f32), axis=1, keepdims=True)
        mark = jnp.where(full >= float(packed), MARK, 0.0)
        place = to_z * ROW + place

    load_text.wait()
    ones = jnp.ones((SLOT, text_v.shape[1]), bf16)
    words = text_v[...].astype(f32)
    squares = words * words
    squares_high = squares.astype(bf16)
    squares_low = (squares - squares_high.astype(f32)).astype(bf16)
    across_lanes = (((1,), (1,)), ((), ()))
    tsq_pair = lax.dot_general(
        ones, squares_high, across_lanes, preferred_element_type=f32
    ) + lax.dot_general(ones, squares_low, across_lanes, preferred_element_type=f32)
    values = jnp.concatenate(
        [
            (local >> 6).astype(f32),
            (local & 63).astype(f32),
            jnp.ones((1, pairs), f32),
            *thirds(tsq_pair[0:1]),
            jnp.zeros((2, pairs), f32),
        ],
        axis=0,
    ).astype(bf16)
    slots = lax.broadcasted_iota(i32, (ROW, pairs), 0)
    taken_rows = {}
    for k in range(NZ):
        pick = one_hot(slots + k * ROW == target)
        meta = lax.dot_general(values, pick, across_lanes, preferred_element_type=f32)
        meta_out[k] = jnp.concatenate(
            [
                meta[0:1] * 64.0 + meta[1:2] + meta[2:3] - 1.0 + mark,
                (meta[3:4] + meta[4:5]) + meta[5:6],
            ],
            axis=0,
        )
        taken_rows[k] = meta[2:3]
        if k == 0 or k in late:
            at = (late.index(k) + 1) if k else 0
            block = jnp.dot(pick, text_v[...], preferred_element_type=f32)
            kept[at] = block.reshape(PLANE, SLOT, -1).astype(bf16)
    if packed:
        filler = jnp.zeros((SLOT - len(late), ROW), f32)
        tile = jnp.concatenate([taken_rows[k] for k in late] + [filler], axis=0)
        taken_out[...] = down(tile).reshape(PLANE, SLOT, ROW).astype(bf16)

    pl.semaphore_wait(barrier, NZ - 1 + PLANE - 1 + 2 * HALF + 3)

    for k in Z_ORDER:
        remote(meta_out.at[k], meta_mid.at[k], mz_send, mz_recv, z_peer[k]).start()
    for i, k in enumerate(first):
        if packed:
            pick = one_hot(slots[0:packed] + k * ROW == place)
        else:
            pick = one_hot(slots + k * ROW == target)
        block = jnp.dot(pick, text_v[...], preferred_element_type=f32)
        sent[i] = block.astype(bf16).reshape(sent.shape[1:])
        remote(sent.at[i], carried.at[i], z_send, z_recv.at[k], z_peer[k]).start()

    def pass_on(source, k):
        for j in range(1, PLANE):
            remote(source.at[j], landed.at[k, j], xy_send, xy_recv.at[k], peer[j]).start()

    if packed:
        for j in range(1, PLANE):
            remote(taken_out.at[j], taken_in.at[j], taken_send, taken_recv, peer[j]).start()
    for i, k in enumerate(late):
        pass_on(kept.at[i + 1], k)
    pass_on(kept.at[0], 0)

    def arrived(k, own):
        settle(landed.at[k, pl.ds(1, PLANE - 1)], xy_recv.at[k])
        return jnp.concatenate(
            [own[0:1].astype(f32), landed[k, 1:PLANE].astype(f32)], axis=0
        ).reshape(ROW, -1)

    over = one_hot(
        lax.broadcasted_iota(i32, (ROW, ROW), 0) < lax.broadcasted_iota(i32, (ROW, ROW), 1)
    )

    def places(taken):
        spot = jnp.dot(one_hot(taken), over, preferred_element_type=f32)
        return jnp.where(taken, spot, -1.0)

    settle(meta_mid.at[pl.ds(1, NZ - 1)], mz_recv)
    metas = [meta_out[0]] + [meta_mid[k] for k in range(1, NZ)]
    tile = jnp.concatenate([m[0:1] for m in metas] + [m[1:2] for m in metas], axis=0)
    if packed:
        tile = jnp.concatenate([tile, places(tile[0:NZ] >= 0.0)], axis=0)
    turned = down(tile)
    meta_tile[...] = turned.reshape(PLANE, SLOT, ROW)
    for j in range(1, PLANE):
        remote(meta_tile.at[j], meta_in.at[j], mt_send, mt_recv, peer[j]).start()
    if packed:
        lanes = lax.broadcasted_iota(i32, (ROW, packed), 1).astype(f32)
        for i, k in enumerate(first):
            at = 2 * NZ + k
            spreaders[i] = one_hot(turned[:, at : at + 1] == lanes)

    def expand_and_pass(i):
        k = first[i]
        settle(carried.at[i], z_recv.at[k])
        if packed:
            block = jnp.dot(spreaders[i], carried[i], preferred_element_type=f32)
            spread[i] = block.reshape(PLANE, SLOT, -1).astype(bf16)
            pass_on(spread.at[i], k)
        else:
            pass_on(carried.at[i], k)

    if packed:
        settle(taken_in.at[pl.ds(1, PLANE - 1)], taken_recv)
        theirs = jnp.concatenate(
            [taken_out[0:1].astype(f32), taken_in[1:PLANE].astype(f32)], axis=0
        ).reshape(ROW, ROW)
        late_place = places(jnp.transpose(theirs)[0:NZ] > 0.5)
        late_rows = lax.broadcasted_iota(i32, (PACKED_LATE, ROW), 0).astype(f32)

    def pack_late(i):
        k = late[i]
        block = arrived(k, kept.at[i + 1]).astype(bf16)
        pick = one_hot(late_rows == late_place[i : i + 1])
        late_sent[i] = jnp.dot(pick, block, preferred_element_type=f32).astype(bf16)
        remote(late_sent.at[i], late_carried.at[i], late_send, z_recv.at[k], z_peer[k]).start()

    for i in range(len(late)):
        pack_late(i)
    expand_and_pass(0)

    settle(meta_in.at[pl.ds(1, PLANE - 1)], mt_recv)
    theirs = jnp.concatenate([meta_tile[0:1], meta_in[1:PLANE]], axis=0).reshape(ROW, ROW)
    by_row = jnp.transpose(theirs)
    slot_ids, tsq_part = by_row[0:NZ], by_row[NZ : 2 * NZ]
    bad = jnp.max(jnp.max(slot_ids, axis=1, keepdims=True), axis=0, keepdims=True) >= MARK * 0.5
    if packed:
        here = places(slot_ids >= 0.0)
        late_here = jnp.concatenate([here[k : k + 1] for k in late], axis=0)
        most = jnp.max(jnp.max(late_here, axis=1, keepdims=True), axis=0, keepdims=True)
        bad = bad | (most >= float(PACKED_LATE))
        turned = down(here)
        lanes = lax.broadcasted_iota(i32, (ROW, PACKED_LATE), 1).astype(f32)
        for i, k in enumerate(late):
            late_spreaders[i] = one_hot(turned[:, k : k + 1] == lanes)
    mark_out[...] = jnp.broadcast_to(jnp.where(bad, 1.0, 0.0), (1, ROW))
    for j in range(1, PLANE):
        remote(mark_out, mark_plane.at[j], mp_send, mp_recv, peer[j]).start()
    for k in range(NZ):
        ids_wide[k] = jnp.broadcast_to(theirs[:, k : k + 1], (ROW, ROW))

    load_table.wait()
    columns = lax.broadcasted_iota(i32, (ROW, ROW), 1)
    columns_f = columns.astype(f32)

    def fetch(k, csq_cols):
        wanted = ids_wide[k]
        for c in range(held // ROW):
            hot[:, c * ROW : (c + 1) * ROW] = one_hot(wanted - float(c * ROW) == columns_f)
        piece = jnp.dot(hot[...], table_v[...], preferred_element_type=f32)
        pieces[k] = piece
        return jnp.where(columns == k, jnp.sum(piece * piece, axis=1, keepdims=True), csq_cols)

    csq_cols = jnp.zeros((ROW, ROW), f32)
    for step in range(4):
        csq_cols = lax.fori_loop(2 * step, 2 * step + 2, fetch, csq_cols)
        if 1 + step < len(first):
            expand_and_pass(1 + step)
    settle(mark_plane.at[pl.ds(1, PLANE - 1)], mp_recv)
    worst = mark_out[...]
    for j in range(1, PLANE):
        worst = jnp.maximum(worst, mark_plane[j])
    mark_sum[...] = worst
    early_out[0] = tsq_part
    early_out[1] = jnp.transpose(csq_cols)[0:NZ]

    remote(early_out.at[1 - core], early_in, e_send.at[0], e_recv.at[0], other_core).start()
    for i in range(5, len(first)):
        expand_and_pass(i)

    for k in Z_ORDER:
        remote(mark_sum, mark_z.at[k], mk_send, mk_recv, z_peer[k]).start()

    dots = jnp.zeros((ROW, ROW), f32)
    for k in (0,) + first + late:
        if k in late:
            i = late.index(k)
            settle(late_carried.at[i], z_recv.at[k])
            words = jnp.dot(late_spreaders[i], late_carried[i], preferred_element_type=f32)
        elif k == 0:
            words = arrived(k, kept.at[0])
        else:
            i = first.index(k)
            words = arrived(k, spread.at[i] if packed else carried.at[i])
        total = jnp.sum(words * pieces[k], axis=1, keepdims=True)
        dots = jnp.where(columns == k, total, dots)
        if k == 0:
            settle(early_in, e_recv.at[0])
            early_sum[0] = early_out[core] + early_in[...]
            early_sum[1] = slot_ids
            remote(early_sum, early_low, e_send.at[1], e_recv.at[1], nearby[HALF]).start()
            remote(
                early_sum.at[0], early_high, e_send.at[2], e_recv.at[2], nearby[-HALF]
            ).start()
    part_out[...] = jnp.transpose(dots)[0:NZ]

    for c in (core, 1 - core):
        remote(part_out, part_in.at[core], part_send, part_recv, ring(HALF, c)).start()
        remote(part_out, part_in.at[2 + core], part_send, part_recv, ring(-HALF, c)).start()
    settle(early_low, e_recv.at[1])
    settle(early_high, e_recv.at[2])
    early_half[...] = early_low[0] + early_high[...]
    mid_ids = early_low[1]
    turned = down(mid_ids)
    for k in range(NZ):
        mid_wide[k] = jnp.broadcast_to(turned[:, k : k + 1], (ROW, ROW))
    remote(early_half, early_other, e_send.at[3], e_recv.at[3], other_core).start()
    settle(mark_z.at[pl.ds(1, NZ - 1)], mk_recv)
    worst = mark_sum[...]
    for k in range(1, NZ):
        worst = jnp.maximum(worst, mark_z[k])
    flag_ref[0] = jnp.where(jnp.max(worst) > 0.5, 1, 0)
    settle(early_other, e_recv.at[3])
    half, other = early_half[...], early_other[...]
    inverse_t = lax.rsqrt(jnp.where(core == 0, half, other) + epsilon)
    inverse_c = lax.rsqrt(jnp.where(core == 0, other, half) + epsilon)
    settle(part_in, part_recv)
    dot = (part_in[0] + part_in[1]) + (part_in[2] + part_in[3])
    match = jax.nn.sigmoid(logit_scale * dot * inverse_t * inverse_c)
    match = jnp.where(mid_ids >= 0.0, match, 0.0)

    match_turned = down(match)
    counts = [jnp.zeros((SLOT, ROW), f32) for _ in range(NZ)]
    for m in range(NZ):
        weight = jnp.broadcast_to(match_turned[:, m : m + 1], (ROW, ROW))
        theirs = mid_wide[m]
        for k in range(NZ):
            same = jnp.where(theirs == mid_ids[k : k + 1], weight, 0.0)
            counts[k] = counts[k] + jnp.sum(same.reshape(ROW // SLOT, SLOT, ROW), axis=0)
    count = jnp.concatenate([jnp.sum(c, axis=0, keepdims=True) for c in counts], axis=0)
    capped = CAP * 1.0
    balanced = match * capped / jnp.maximum(count, capped)

    for k in range(NZ):
        back_out[(k + HALF) % NZ] = balanced[k : k + 1]
    for k in (0, 7, 1, 6, 2, 5, 3):
        i = (k + HALF) % NZ
        remote(back_out.at[i], back_mid.at[i], bz_send, bz_recv, nearby[HALF - k]).start()
    settle(back_mid.at[pl.ds(1, NZ - 1)], bz_recv)
    back_tile[...] = jnp.concatenate(
        [back_out[0] if k == HALF else back_mid[(k + HALF) % NZ] for k in range(NZ)], axis=0
    )
    for j in range(1, PLANE):
        remote(back_tile, back_in.at[j], bt_send, bt_recv, peer_back[j]).start()
    at_slot = one_hot(slots == lane)
    settle(back_in.at[pl.ds(1, PLANE - 1)], bt_recv)
    group = lax.broadcasted_iota(i32, (NZ, ROW), 1) // SLOT
    given = back_tile[...]
    for j in range(1, PLANE):
        given = jnp.where(group == j, back_in[j], given)
    looked = jnp.dot(
        jnp.concatenate(thirds(given), axis=0).astype(bf16), at_slot, preferred_element_type=f32
    )
    looked = (looked[0:NZ] + looked[NZ : 2 * NZ]) + looked[2 * NZ : 3 * NZ]
    at_block = lax.broadcasted_iota(i32, (NZ, pairs), 0)
    out_ref[...] = jnp.sum(jnp.where(at_block == to_z, looked, 0.0), axis=0, keepdims=True)

    settle(meta_out.at[pl.ds(1, NZ - 1)], mz_send)
    settle(sent, z_send)
    if packed:
        settle(late_sent, late_send)
        settle(taken_in.at[pl.ds(1, PLANE - 1)], taken_send)
    settle(landed.at[:, pl.ds(1, PLANE - 1)], xy_send)
    settle(meta_in.at[pl.ds(1, PLANE - 1)], mt_send)
    settle(early_in, e_send.at[0])
    settle(early_other, e_send.at[3])
    settle(mark_plane.at[pl.ds(1, PLANE - 1)], mp_send)
    settle(mark_z.at[pl.ds(1, NZ - 1)], mk_send)
    settle(early_low, e_send.at[1])
    settle(early_high, e_send.at[2])
    settle(part_in, part_send)
    settle(back_out.at[pl.ds(1, NZ - 1)], bz_send)
    settle(back_in.at[pl.ds(1, PLANE - 1)], bt_send)


def curate(packed, text, concept_table, ids):
    pairs, quarter = text.shape
    held = concept_table.shape[0]
    vmem, dma = pltpu.VMEM, pltpu.SemaphoreType.DMA
    blocks = (NZ, PLANE, SLOT, quarter)
    piece = (PLANE, SLOT, quarter)
    fast, slow = len(Z_FIRST), len(PLANE_FIRST)
    moved = (fast, packed, quarter) if packed else (NZ - 1, *piece)
    return pl.pallas_call(
        functools.partial(kernel, packed),
        name="curate_packed" if packed else "curate_whole",
        out_shape=(
            jax.ShapeDtypeStruct((1, pairs), f32),
            pltpu.SMEM((1,), i32),
        ),
        in_specs=[
            pl.BlockSpec(memory_space=pl.ANY),
            pl.BlockSpec(memory_space=pl.ANY),
            pl.BlockSpec(memory_space=pl.ANY),
        ],
        out_specs=(
            pl.BlockSpec(memory_space=pltpu.VMEM),
            pl.BlockSpec(memory_space=pltpu.SMEM),
        ),
        scratch_shapes=[
            vmem((1, pairs), i32),
            vmem((pairs, quarter), bf16),
            vmem((held, quarter), bf16),
            vmem((1 + slow if packed else 1, *piece), bf16),
            vmem(moved, bf16),
            vmem(moved, bf16),
            vmem((fast, *piece) if packed else (1, 1, SLOT, quarter), bf16),
            vmem((fast, ROW, packed) if packed else (1, SLOT, ROW), bf16),
            vmem(blocks, bf16),
            vmem((slow, PACKED_LATE, quarter), bf16),
            vmem((slow, PACKED_LATE, quarter), bf16),
            vmem((slow, ROW, PACKED_LATE), bf16),
            vmem((PLANE, SLOT, ROW), bf16),
            vmem((PLANE, SLOT, ROW), bf16),
            vmem((NZ, 2, ROW), f32),
            vmem((NZ, 2, ROW), f32),
            vmem((PLANE, SLOT, ROW), f32),
            vmem((PLANE, SLOT, ROW), f32),
            vmem((NZ, ROW, ROW), f32),
            vmem((ROW, held), bf16),
            vmem((NZ, ROW, quarter), f32),
            vmem((2, NZ, ROW), f32),
            vmem((NZ, ROW), f32),
            vmem((2, NZ, ROW), f32),
            vmem((2, NZ, ROW), f32),
            vmem((NZ, ROW), f32),
            vmem((NZ, ROW), f32),
            vmem((NZ, ROW), f32),
            vmem((NZ, ROW, ROW), f32),
            vmem((1, ROW), f32),
            vmem((PLANE, 1, ROW), f32),
            vmem((1, ROW), f32),
            vmem((NZ, 1, ROW), f32),
            vmem((NZ, ROW), f32),
            vmem((4, NZ, ROW), f32),
            vmem((NZ, 1, ROW), f32),
            vmem((NZ, 1, ROW), f32),
            vmem((NZ, ROW), f32),
            vmem((PLANE, NZ, ROW), f32),
            dma((3,)),
            dma, dma((NZ,)), dma, dma, dma, dma, dma, dma((NZ,)),
            dma((4,)), dma((4,)), dma, dma, dma, dma, dma, dma,
            dma, dma, dma, dma, dma, dma, dma,
        ],
        compiler_params=pltpu.CompilerParams(
            collective_id=1 if packed else 0, has_side_effects=True
        ),
    )(text, concept_table, ids)


def body(text, concept_table, ids):
    pairs = text.shape[0]
    line = ids.reshape(1, pairs)
    out, over = curate(PACKED, text, concept_table, line)
    out = lax.cond(
        over[0] > 0,
        lambda: curate(0, text, concept_table, line)[0],
        lambda: out,
    )
    return out.reshape(pairs)


def solution(mesh):
    placed = (P("dp", "concept"), P("dp", "concept"), P("dp"))
    return jax.shard_map(body, mesh=mesh, in_specs=placed, out_specs=P("dp"), check_vma=False)
```

```python
import functools

import jax
import jax.numpy as jnp
from jax import lax
from jax.experimental import pallas as pl
from jax.experimental.pallas import tpu as pltpu
from jax.sharding import PartitionSpec as P

CAP = 16
SLOT = 8
NX, NZ, NY = 4, 8, 4
PLANE = NX * NY
ROW = PLANE * SLOT
Z_ORDER = (4, 3, 5, 2, 6, 1, 7)
Z_FIRST = (4,)
PLANE_FIRST = (3, 5, 2, 6, 1, 7)
PACKED = 88
PACKED_LATE = 96
MARK = 8192.0
HALF = NZ // 2

logit_scale = 64.0
epsilon = 1e-06
f32, bf16, i32 = jnp.float32, jnp.bfloat16, jnp.int32


def one_hot(test):
    return jnp.where(test, 1.0, 0.0).astype(bf16)


def thirds(x):
    high = x.astype(bf16).astype(f32)
    middle = (x - high).astype(bf16).astype(f32)
    low = x - high - middle
    return [high, middle, low]


def down(square):
    filler = jnp.zeros((ROW - square.shape[0], ROW), f32)
    return jnp.transpose(jnp.concatenate([square, filler], axis=0))


def kernel(
    packed, text_hbm, table_hbm, ids_hbm, out_ref, flag_ref,
    ids_ref, text_v, table_v, kept, sent, carried, spread, spreaders, landed,
    late_sent, late_carried, late_spreaders, taken_out, taken_in,
    meta_out, meta_mid, meta_tile, meta_in, ids_wide, hot, pieces,
    early_out, early_in, early_sum, early_low, early_high, early_half, early_other, mid_wide,
    mark_out, mark_plane, mark_sum, mark_z,
    part_out, part_in, back_out, back_mid, back_tile, back_in,
    load_sem, z_send, z_recv, mz_send, mz_recv, mt_send, mt_recv, xy_send, xy_recv,
    e_send, e_recv, part_send, part_recv, bz_send, bz_recv, bt_send, bt_recv,
    late_send, taken_send, taken_recv, mp_send, mp_recv, mk_send, mk_recv,
):
    pairs = ids_ref.shape[1]
    held = table_v.shape[0]
    first = Z_FIRST if packed else Z_ORDER
    late = PLANE_FIRST if packed else ()
    me = lax.axis_index("dp")
    mine = lax.axis_index("concept")
    my_x, my_z, my_y = lax.div(me, NZ * NY), lax.rem(lax.div(me, NY), NZ), lax.rem(me, NY)
    core = lax.rem(mine, 2)
    partner = mine + 1 - 2 * core
    my_ring = lax.div(mine, 2) * NZ + my_z

    z_peer = [(me + (lax.rem(my_z + k, NZ) - my_z) * NY, mine) for k in range(NZ)]
    x_step = [(lax.rem(my_x + d, NX) - my_x) * (NZ * NY) for d in range(NX)]
    y_step = [lax.rem(my_y + d, NY) - my_y for d in range(NY)]
    peer = [(me + x_step[j // NY] + y_step[j % NY], mine) for j in range(PLANE)]
    peer_back = [peer[(-(j // NY)) % NX * NY + (-j) % NY] for j in range(PLANE)]
    other_core = (me, partner)

    def ring(step, on_core):
        there = lax.rem(my_ring + step + 2 * NZ, 2 * NZ)
        return (me + (lax.rem(there, NZ) - my_z) * NY, lax.div(there, NZ) * 2 + on_core)

    nearby = {e: ring(e, core) for e in range(-HALF, HALF + 1)}

    def remote(src, dst, send, recv, device):
        return pltpu.make_async_remote_copy(
            src_ref=src, dst_ref=dst, send_sem=send, recv_sem=recv,
            device_id=device, device_id_type=pl.DeviceIdType.MESH,
        )

    def settle(ref, sem):
        pltpu.make_async_copy(ref, ref, sem).wait()

    barrier = pltpu.get_barrier_semaphore()

    def greet(device):
        pl.semaphore_signal(
            barrier, inc=1, device_id=device, device_id_type=pl.DeviceIdType.MESH
        )

    load_text = pltpu.make_async_copy(text_hbm, text_v, load_sem.at[0])
    load_ids = pltpu.make_async_copy(ids_hbm, ids_ref, load_sem.at[2])
    load_ids.start()
    for k in Z_ORDER:
        greet(z_peer[k])
    for j in range(1, PLANE):
        greet(peer[j])
    for e in range(1, HALF + 1):
        greet(nearby[e])
        greet(nearby[-e])
    greet(ring(HALF, 1 - core))
    greet(ring(-HALF, 1 - core))
    greet(other_core)
    load_text.start()
    load_table = pltpu.make_async_copy(table_hbm, table_v, load_sem.at[1])
    load_table.start()

    load_ids.wait()
    ids = ids_ref[...]
    owner = ((ids >> 10) * 43691) >> 17
    local = ids - owner * held
    to_z = (((owner >> 2) & 7) - my_z) & 7
    to_plane = ((((owner >> 5) - my_x) & 3) << 2) | (((owner & 3) - my_y) & 3)
    relative = to_z * PLANE + to_plane
    owners = lax.broadcasted_iota(i32, (NZ * PLANE, pairs), 0)
    is_owner = jnp.where(owners == relative, 1.0, 0.0)
    earlier = one_hot(
        lax.broadcasted_iota(i32, (pairs, pairs), 0)
        < lax.broadcasted_iota(i32, (pairs, pairs), 1)
    )
    is_owner_low = is_owner.astype(bf16)
    ahead = jnp.dot(is_owner_low, earlier, preferred_element_type=f32)
    rank = jnp.sum(is_owner * ahead, axis=0, keepdims=True).astype(i32)
    lane = to_plane * SLOT + rank
    target = to_z * ROW + lane
    mark = 0.0
    if packed:
        down_i = lax.broadcasted_iota(i32, (NZ * PLANE, NZ * PLANE), 0)
        over_i = lax.broadcasted_iota(i32, (NZ * PLANE, NZ * PLANE), 1)
        before = one_hot((over_i < down_i) & ((over_i >> 4) == (down_i >> 4)))
        held_by = jnp.sum(is_owner, axis=1, keepdims=True)
        held_by = jnp.broadcast_to(held_by, (NZ * PLANE, ROW)).astype(bf16)
        base = jnp.dot(before, held_by, preferred_element_type=f32)[:, 0:1]
        place = rank + jnp.sum(is_owner * base, axis=0, keepdims=True).astype(i32)
        full = jnp.max(place.astype(f32), axis=1, keepdims=True)
        mark = jnp.where(full >= float(packed), MARK, 0.0)
        place = to_z * ROW + place

    load_text.wait()
    ones = jnp.ones((SLOT, text_v.shape[1]), bf16)
    words = text_v[...].astype(f32)
    squares = words * words
    squares_high = squares.astype(bf16)
    squares_low = (squares - squares_high.astype(f32)).astype(bf16)
    across_lanes = (((1,), (1,)), ((), ()))
    tsq_pair = lax.dot_general(
        ones, squares_high, across_lanes, preferred_element_type=f32
    ) + lax.dot_general(ones, squares_low, across_lanes, preferred_element_type=f32)
    values = jnp.concatenate(
        [
            (local >> 6).astype(f32),
            (local & 63).astype(f32),
            jnp.ones((1, pairs), f32),
            *thirds(tsq_pair[0:1]),
            jnp.zeros((2, pairs), f32),
        ],
        axis=0,
    ).astype(bf16)
    slots = lax.broadcasted_iota(i32, (ROW, pairs), 0)
    taken_rows = {}
    for k in range(NZ):
        pick = one_hot(slots + k * ROW == target)
        meta = lax.dot_general(values, pick, across_lanes, preferred_element_type=f32)
        meta_out[k] = jnp.concatenate(
            [
                meta[0:1] * 64.0 + meta[1:2] + meta[2:3] - 1.0 + mark,
                (meta[3:4] + meta[4:5]) + meta[5:6],
            ],
            axis=0,
        )
        taken_rows[k] = meta[2:3]
        if k == 0 or k in late:
            at = (late.index(k) + 1) if k else 0
            block = jnp.dot(pick, text_v[...], preferred_element_type=f32)
            kept[at] = block.reshape(PLANE, SLOT, -1).astype(bf16)
    if packed:
        filler = jnp.zeros((SLOT - len(late), ROW), f32)
        tile = jnp.concatenate([taken_rows[k] for k in late] + [filler], axis=0)
        taken_out[...] = down(tile).reshape(PLANE, SLOT, ROW).astype(bf16)

    pl.semaphore_wait(barrier, NZ - 1 + PLANE - 1 + 2 * HALF + 3)

    for k in Z_ORDER:
        remote(meta_out.at[k], meta_mid.at[k], mz_send, mz_recv, z_peer[k]).start()
    for i, k in enumerate(first):
        if packed:
            pick = one_hot(slots[0:packed] + k * ROW == place)
        else:
            pick = one_hot(slots + k * ROW == target)
        block = jnp.dot(pick, text_v[...], preferred_element_type=f32)
        sent[i] = block.astype(bf16).reshape(sent.shape[1:])
        remote(sent.at[i], carried.at[i], z_send, z_recv.at[k], z_peer[k]).start()

    def pass_on(source, k):
        for j in range(1, PLANE):
            remote(source.at[j], landed.at[k, j], xy_send, xy_recv.at[k], peer[j]).start()

    if packed:
        for j in range(1, PLANE):
            remote(taken_out.at[j], taken_in.at[j], taken_send, taken_recv, peer[j]).start()
    for i, k in enumerate(late):
        pass_on(kept.at[i + 1], k)
    pass_on(kept.at[0], 0)

    def arrived(k, own):
        settle(landed.at[k, pl.ds(1, PLANE - 1)], xy_recv.at[k])
        return jnp.concatenate(
            [own[0:1].astype(f32), landed[k, 1:PLANE].astype(f32)], axis=0
        ).reshape(ROW, -1)

    over = one_hot(
        lax.broadcasted_iota(i32, (ROW, ROW), 0) < lax.broadcasted_iota(i32, (ROW, ROW), 1)
    )

    def places(taken):
        spot = jnp.dot(one_hot(taken), over, preferred_element_type=f32)
        return jnp.where(taken, spot, -1.0)

    if packed:
        settle(taken_in.at[pl.ds(1, PLANE - 1)], taken_recv)
        theirs = jnp.concatenate(
            [taken_out[0:1].astype(f32), taken_in[1:PLANE].astype(f32)], axis=0
        ).reshape(ROW, ROW)
        late_place = places(jnp.transpose(theirs)[0:NZ] > 0.5)
        late_rows = lax.broadcasted_iota(i32, (PACKED_LATE, ROW), 0).astype(f32)

    def pack_late(i):
        k = late[i]
        block = arrived(k, kept.at[i + 1]).astype(bf16)
        pick = one_hot(late_rows == late_place[i : i + 1])
        late_sent[i] = jnp.dot(pick, block, preferred_element_type=f32).astype(bf16)
        remote(late_sent.at[i], late_carried.at[i], late_send, z_recv.at[k], z_peer[k]).start()

    for i in range(min(2, len(late))):
        pack_late(i)

    settle(meta_mid.at[pl.ds(1, NZ - 1)], mz_recv)
    metas = [meta_out[0]] + [meta_mid[k] for k in range(1, NZ)]
    tile = jnp.concatenate([m[0:1] for m in metas] + [m[1:2] for m in metas], axis=0)
    if packed:
        tile = jnp.concatenate([tile, places(tile[0:NZ] >= 0.0)], axis=0)
    turned = down(tile)
    meta_tile[...] = turned.reshape(PLANE, SLOT, ROW)
    for j in range(1, PLANE):
        remote(meta_tile.at[j], meta_in.at[j], mt_send, mt_recv, peer[j]).start()
    if packed:
        lanes = lax.broadcasted_iota(i32, (ROW, packed), 1).astype(f32)
        for i, k in enumerate(first):
            at = 2 * NZ + k
            spreaders[i] = one_hot(turned[:, at : at + 1] == lanes)

    def expand_and_pass(i):
        k = first[i]
        settle(carried.at[i], z_recv.at[k])
        if packed:
            block = jnp.dot(spreaders[i], carried[i], preferred_element_type=f32)
            spread[i] = block.reshape(PLANE, SLOT, -1).astype(bf16)
            pass_on(spread.at[i], k)
        else:
            pass_on(carried.at[i], k)

    for i in range(2, len(late)):
        pack_late(i)
    expand_and_pass(0)

    settle(meta_in.at[pl.ds(1, PLANE - 1)], mt_recv)
    theirs = jnp.concatenate([meta_tile[0:1], meta_in[1:PLANE]], axis=0).reshape(ROW, ROW)
    by_row = jnp.transpose(theirs)
    slot_ids, tsq_part = by_row[0:NZ], by_row[NZ : 2 * NZ]
    bad = jnp.max(jnp.max(slot_ids, axis=1, keepdims=True), axis=0, keepdims=True) >= MARK * 0.5
    if packed:
        here = places(slot_ids >= 0.0)
        late_here = jnp.concatenate([here[k : k + 1] for k in late], axis=0)
        most = jnp.max(jnp.max(late_here, axis=1, keepdims=True), axis=0, keepdims=True)
        bad = bad | (most >= float(PACKED_LATE))
        turned = down(here)
        lanes = lax.broadcasted_iota(i32, (ROW, PACKED_LATE), 1).astype(f32)
        for i, k in enumerate(late):
            late_spreaders[i] = one_hot(turned[:, k : k + 1] == lanes)
    mark_out[...] = jnp.broadcast_to(jnp.where(bad, 1.0, 0.0), (1, ROW))
    for j in range(1, PLANE):
        remote(mark_out, mark_plane.at[j], mp_send, mp_recv, peer[j]).start()
    for k in range(NZ):
        ids_wide[k] = jnp.broadcast_to(theirs[:, k : k + 1], (ROW, ROW))

    load_table.wait()
    columns = lax.broadcasted_iota(i32, (ROW, ROW), 1)
    columns_f = columns.astype(f32)

    def fetch(k, csq_cols):
        wanted = ids_wide[k]
        for c in range(held // ROW):
            hot[:, c * ROW : (c + 1) * ROW] = one_hot(wanted - float(c * ROW) == columns_f)
        piece = jnp.dot(hot[...], table_v[...], preferred_element_type=f32)
        pieces[k] = piece
        return jnp.where(columns == k, jnp.sum(piece * piece, axis=1, keepdims=True), csq_cols)

    csq_cols = jnp.zeros((ROW, ROW), f32)
    for step in range(4):
        csq_cols = lax.fori_loop(2 * step, 2 * step + 2, fetch, csq_cols)
        if 1 + step < len(first):
            expand_and_pass(1 + step)
    settle(mark_plane.at[pl.ds(1, PLANE - 1)], mp_recv)
    worst = mark_out[...]
    for j in range(1, PLANE):
        worst = jnp.maximum(worst, mark_plane[j])
    mark_sum[...] = worst
    early_out[0] = tsq_part
    early_out[1] = jnp.transpose(csq_cols)[0:NZ]

    remote(early_out.at[1 - core], early_in, e_send.at[0], e_recv.at[0], other_core).start()
    for i in range(5, len(first)):
        expand_and_pass(i)

    for k in Z_ORDER:
        remote(mark_sum, mark_z.at[k], mk_send, mk_recv, z_peer[k]).start()

    dots = jnp.zeros((ROW, ROW), f32)
    for k in (0,) + first + late:
        if k in late:
            i = late.index(k)
            settle(late_carried.at[i], z_recv.at[k])
            words = jnp.dot(late_spreaders[i], late_carried[i], preferred_element_type=f32)
        elif k == 0:
            words = arrived(k, kept.at[0])
        else:
            i = first.index(k)
            words = arrived(k, spread.at[i] if packed else carried.at[i])
        total = jnp.sum(words * pieces[k], axis=1, keepdims=True)
        dots = jnp.where(columns == k, total, dots)
        if k == 0:
            settle(early_in, e_recv.at[0])
            early_sum[0] = early_out[core] + early_in[...]
            early_sum[1] = slot_ids
            remote(early_sum, early_low, e_send.at[1], e_recv.at[1], nearby[HALF]).start()
            remote(
                early_sum.at[0], early_high, e_send.at[2], e_recv.at[2], nearby[-HALF]
            ).start()
    part_out[...] = jnp.transpose(dots)[0:NZ]

    for c in (core, 1 - core):
        remote(part_out, part_in.at[core], part_send, part_recv, ring(HALF, c)).start()
        remote(part_out, part_in.at[2 + core], part_send, part_recv, ring(-HALF, c)).start()
    settle(early_low, e_recv.at[1])
    settle(early_high, e_recv.at[2])
    early_half[...] = early_low[0] + early_high[...]
    mid_ids = early_low[1]
    turned = down(mid_ids)
    for k in range(NZ):
        mid_wide[k] = jnp.broadcast_to(turned[:, k : k + 1], (ROW, ROW))
    remote(early_half, early_other, e_send.at[3], e_recv.at[3], other_core).start()
    settle(mark_z.at[pl.ds(1, NZ - 1)], mk_recv)
    worst = mark_sum[...]
    for k in range(1, NZ):
        worst = jnp.maximum(worst, mark_z[k])
    flag_ref[0] = jnp.where(jnp.max(worst) > 0.5, 1, 0)
    settle(early_other, e_recv.at[3])
    half, other = early_half[...], early_other[...]
    inverse_t = lax.rsqrt(jnp.where(core == 0, half, other) + epsilon)
    inverse_c = lax.rsqrt(jnp.where(core == 0, other, half) + epsilon)
    settle(part_in, part_recv)
    dot = (part_in[0] + part_in[1]) + (part_in[2] + part_in[3])
    match = jax.nn.sigmoid(logit_scale * dot * inverse_t * inverse_c)
    match = jnp.where(mid_ids >= 0.0, match, 0.0)

    match_turned = down(match)
    counts = [jnp.zeros((SLOT, ROW), f32) for _ in range(NZ)]
    for m in range(NZ):
        weight = jnp.broadcast_to(match_turned[:, m : m + 1], (ROW, ROW))
        theirs = mid_wide[m]
        for k in range(NZ):
            same = jnp.where(theirs == mid_ids[k : k + 1], weight, 0.0)
            counts[k] = counts[k] + jnp.sum(same.reshape(ROW // SLOT, SLOT, ROW), axis=0)
    count = jnp.concatenate([jnp.sum(c, axis=0, keepdims=True) for c in counts], axis=0)
    capped = CAP * 1.0
    balanced = match * capped / jnp.maximum(count, capped)

    for k in range(NZ):
        back_out[(k + HALF) % NZ] = balanced[k : k + 1]
    for k in (0, 7, 1, 6, 2, 5, 3):
        i = (k + HALF) % NZ
        remote(back_out.at[i], back_mid.at[i], bz_send, bz_recv, nearby[HALF - k]).start()
    settle(back_mid.at[pl.ds(1, NZ - 1)], bz_recv)
    back_tile[...] = jnp.concatenate(
        [back_out[0] if k == HALF else back_mid[(k + HALF) % NZ] for k in range(NZ)], axis=0
    )
    for j in range(1, PLANE):
        remote(back_tile, back_in.at[j], bt_send, bt_recv, peer_back[j]).start()
    at_slot = one_hot(slots == lane)
    settle(back_in.at[pl.ds(1, PLANE - 1)], bt_recv)
    group = lax.broadcasted_iota(i32, (NZ, ROW), 1) // SLOT
    given = back_tile[...]
    for j in range(1, PLANE):
        given = jnp.where(group == j, back_in[j], given)
    looked = jnp.dot(
        jnp.concatenate(thirds(given), axis=0).astype(bf16), at_slot, preferred_element_type=f32
    )
    looked = (looked[0:NZ] + looked[NZ : 2 * NZ]) + looked[2 * NZ : 3 * NZ]
    at_block = lax.broadcasted_iota(i32, (NZ, pairs), 0)
    out_ref[...] = jnp.sum(jnp.where(at_block == to_z, looked, 0.0), axis=0, keepdims=True)

    settle(meta_out.at[pl.ds(1, NZ - 1)], mz_send)
    settle(sent, z_send)
    if packed:
        settle(late_sent, late_send)
        settle(taken_in.at[pl.ds(1, PLANE - 1)], taken_send)
    settle(landed.at[:, pl.ds(1, PLANE - 1)], xy_send)
    settle(meta_in.at[pl.ds(1, PLANE - 1)], mt_send)
    settle(early_in, e_send.at[0])
    settle(early_other, e_send.at[3])
    settle(mark_plane.at[pl.ds(1, PLANE - 1)], mp_send)
    settle(mark_z.at[pl.ds(1, NZ - 1)], mk_send)
    settle(early_low, e_send.at[1])
    settle(early_high, e_send.at[2])
    settle(part_in, part_send)
    settle(back_out.at[pl.ds(1, NZ - 1)], bz_send)
    settle(back_in.at[pl.ds(1, PLANE - 1)], bt_send)


def curate(packed, text, concept_table, ids):
    pairs, quarter = text.shape
    held = concept_table.shape[0]
    vmem, dma = pltpu.VMEM, pltpu.SemaphoreType.DMA
    blocks = (NZ, PLANE, SLOT, quarter)
    piece = (PLANE, SLOT, quarter)
    fast, slow = len(Z_FIRST), len(PLANE_FIRST)
    moved = (fast, packed, quarter) if packed else (NZ - 1, *piece)
    return pl.pallas_call(
        functools.partial(kernel, packed),
        name="curate_packed" if packed else "curate_whole",
        out_shape=(
            jax.ShapeDtypeStruct((1, pairs), f32),
            pltpu.SMEM((1,), i32),
        ),
        in_specs=[
            pl.BlockSpec(memory_space=pl.ANY),
            pl.BlockSpec(memory_space=pl.ANY),
            pl.BlockSpec(memory_space=pl.ANY),
        ],
        out_specs=(
            pl.BlockSpec(memory_space=pltpu.VMEM),
            pl.BlockSpec(memory_space=pltpu.SMEM),
        ),
        scratch_shapes=[
            vmem((1, pairs), i32),
            vmem((pairs, quarter), bf16),
            vmem((held, quarter), bf16),
            vmem((1 + slow if packed else 1, *piece), bf16),
            vmem(moved, bf16),
            vmem(moved, bf16),
            vmem((fast, *piece) if packed else (1, 1, SLOT, quarter), bf16),
            vmem((fast, ROW, packed) if packed else (1, SLOT, ROW), bf16),
            vmem(blocks, bf16),
            vmem((slow, PACKED_LATE, quarter), bf16),
            vmem((slow, PACKED_LATE, quarter), bf16),
            vmem((slow, ROW, PACKED_LATE), bf16),
            vmem((PLANE, SLOT, ROW), bf16),
            vmem((PLANE, SLOT, ROW), bf16),
            vmem((NZ, 2, ROW), f32),
            vmem((NZ, 2, ROW), f32),
            vmem((PLANE, SLOT, ROW), f32),
            vmem((PLANE, SLOT, ROW), f32),
            vmem((NZ, ROW, ROW), f32),
            vmem((ROW, held), bf16),
            vmem((NZ, ROW, quarter), f32),
            vmem((2, NZ, ROW), f32),
            vmem((NZ, ROW), f32),
            vmem((2, NZ, ROW), f32),
            vmem((2, NZ, ROW), f32),
            vmem((NZ, ROW), f32),
            vmem((NZ, ROW), f32),
            vmem((NZ, ROW), f32),
            vmem((NZ, ROW, ROW), f32),
            vmem((1, ROW), f32),
            vmem((PLANE, 1, ROW), f32),
            vmem((1, ROW), f32),
            vmem((NZ, 1, ROW), f32),
            vmem((NZ, ROW), f32),
            vmem((4, NZ, ROW), f32),
            vmem((NZ, 1, ROW), f32),
            vmem((NZ, 1, ROW), f32),
            vmem((NZ, ROW), f32),
            vmem((PLANE, NZ, ROW), f32),
            dma((3,)),
            dma, dma((NZ,)), dma, dma, dma, dma, dma, dma((NZ,)),
            dma((4,)), dma((4,)), dma, dma, dma, dma, dma, dma,
            dma, dma, dma, dma, dma, dma, dma,
        ],
        compiler_params=pltpu.CompilerParams(
            collective_id=1 if packed else 0, has_side_effects=True
        ),
    )(text, concept_table, ids)


def body(text, concept_table, ids):
    pairs = text.shape[0]
    line = ids.reshape(1, pairs)
    out, over = curate(PACKED, text, concept_table, line)
    out = lax.cond(
        over[0] > 0,
        lambda: curate(0, text, concept_table, line)[0],
        lambda: out,
    )
    return out.reshape(pairs)


def solution(mesh):
    placed = (P("dp", "concept"), P("dp", "concept"), P("dp"))
    return jax.shard_map(body, mesh=mesh, in_specs=placed, out_specs=P("dp"), check_vma=False)
```
